8 devices in a mesh: col: 4 (over z, y, x), row: 2 (over core).
Axes of the slice: x: 2, y: 2, z: 1, core: 2. Of those that a mesh axis runs over, the one named last changes fastest.
Arguments:
- matrix: bfloat16 [11264, 11264], P('row', 'col')
- y_start: float32 [11264, 64], P(('col', 'row'))
- center: float32 [], replicated
- half_width: float32 [], replicated
Outputs:
- output 1: float32 [11264, 64], P(('col', 'row'))
- output 2: float32 [64, 64], replicated
All inputs are finite; a program needn't handle non-finite values.
Results may differ from the reference program's by a relative error of at most 0.0144715.
Values are sent between devices in bfloat16 or wider.
A program may use at most 1 GiB of HBM per device.

```python
import jax
import jax.numpy as jnp
from jax import lax

N = 11264
WIDTH = 64
DEGREE = 8


def setup_inputs(seed: int = 0) -> dict:
    root_key = jax.random.key(seed)
    key_mat, key_vec, key_center, key_width = jax.random.split(root_key, 4)
    base_draw = jax.random.normal(key_mat, (N, N), jnp.float32)
    matrix = ((base_draw + base_draw.T) * (2.0 * N) ** -0.5).astype(jnp.bfloat16)
    y_start = jax.random.normal(key_vec, (N, WIDTH), jnp.float32)
    center = jax.random.uniform(key_center, (), jnp.float32, -0.5, 0.5)
    half_width = 2.3 + jnp.abs(center) + jax.random.uniform(key_width, (), jnp.float32, 0.0, 0.5)
    return {"matrix": matrix, "y_start": y_start, "center": center, "half_width": half_width}


def apply_matrix(matrix, vectors):
    return jnp.dot(matrix, vectors.astype(jnp.bfloat16), preferred_element_type=jnp.float32)


def reference(matrix, y_start, center, half_width):
    y_first = (apply_matrix(matrix, y_start) - center * y_start) / half_width

    def sweep_step(state_pair, unused):
        y_prev, y_cur = state_pair
        y_next = 2.0 * (apply_matrix(matrix, y_cur) - center * y_cur) / half_width - y_prev
        return (y_cur, y_next), unused

    final_pair, unused_out = lax.scan(sweep_step, (y_start, y_first), None, length=DEGREE - 1)
    y_last = final_pair[1]
    y_low = y_last.astype(jnp.bfloat16)
    image_low = apply_matrix(matrix, y_last).astype(jnp.bfloat16)
    gram_mat = jnp.dot(y_low.T, image_low, preferred_element_type=jnp.float32) / N
    return y_last, gram_mat
```

```python
import functools

import jax
import jax.numpy as jnp
from jax import lax
from jax.experimental import pallas as pl
from jax.experimental.pallas import tpu as pltpu
from jax.sharding import PartitionSpec as P

DEGREE = 8
WIDTHS = (512, 512, 384)
OFFSETS = (0, 512, 1024)
CHUNKS = len(WIDTHS)
MESH = pl.DeviceIdType.MESH


def filter_kernel(piece, width, a_ref, y0_ref, c_ref, e_ref, y_out, g_out, tile, src, state, acc, psend, prec, gall, tile_sem, recv_sem, send_sem, fwd_sem, psend_sem, prec_sem, gsend_sem, grecv_sem, y_sem):
    chip = lax.axis_index("col")
    core = lax.axis_index("row")
    me = chip * 2 + core
    sibling = 1 - core
    chip_bit = lax.rem(chip, 2)
    chip_x = chip + 1 - 2 * chip_bit
    chip_y = lax.rem(chip + 2, 4)
    group = chip // 2
    near = core == group
    far = core != group
    near_int = 1 - lax.abs(core - group)

    own_dest = 2 * chip_bit + core
    own_slot = near_int * own_dest + (1 - near_int) * 4
    pair_first = 2 * chip_bit
    pair_second = 2 * (1 - chip_bit)
    fwd_slot = near_int * pair_second + (1 - near_int) * (pair_first + 1)
    fwd_chip = near_int * chip_y + (1 - near_int) * chip_x
    sib_slot = pair_first + sibling

    def local_load(order, slot, half):
        col = half * core + (1 - half) * sibling
        c = order
        rows = pl.ds(pl.multiple_of(slot * piece + OFFSETS[c], 128), WIDTHS[c])
        return pltpu.make_async_copy(
            a_ref.at[rows, pl.ds(pl.multiple_of(col * piece, 128), piece)],
            tile.at[rows, pl.ds(half * piece, piece)],
            tile_sem.at[slot, c, half],
        )

    def slot_view(par, slot, c):
        return src.at[par, slot, :, pl.ds(OFFSETS[c], WIDTHS[c])]

    def remote(src_view, dst_view, ssem, rsem, dev):
        return pltpu.make_async_remote_copy(src_ref=src_view, dst_ref=dst_view, send_sem=ssem, recv_sem=rsem, device_id=dev, device_id_type=MESH)

    def own_copy(par, c, d):
        dev = ((chip_x, group), (chip_y, group), (chip, group))[d]
        return remote(slot_view(par, own_slot, c), slot_view(par, own_dest, c), send_sem.at[d, c], recv_sem.at[par, own_dest, c], dev)

    def fwd_copy(par, c):
        return remote(slot_view(par, fwd_slot, c), slot_view(par, fwd_slot, c), fwd_sem.at[c], recv_sem.at[par, fwd_slot, c], (fwd_chip, core))

    def wait_slot(par, slot, c):
        view = slot_view(par, slot, c)
        remote(view, view, fwd_sem.at[c], recv_sem.at[par, slot, c], (chip, core)).wait_recv()

    def partial_copy(par, o):
        cols = pl.ds(OFFSETS[o], WIDTHS[o])
        return remote(psend.at[:, cols], prec.at[par, :, cols], psend_sem.at[o], prec_sem.at[par, o], (chip, sibling))

    def send_own(par, c):
        own_copy(par, c, 0).start()
        own_copy(par, c, 1).start()

        @pl.when(far)
        def _():
            own_copy(par, c, 2).start()

    def wait_own_sends(par, c):
        own_copy(par, c, 0).wait_send()
        own_copy(par, c, 1).wait_send()

        @pl.when(far)
        def _():
            own_copy(par, c, 2).wait_send()

    for pair in (pair_first, pair_second):
        for c in range(CHUNKS):
            for k in range(2):
                for half in range(2):
                    local_load(c, pair + k, half).start()

    barrier = pltpu.get_barrier_semaphore()
    for d in range(1, 8):
        other = lax.rem(me + d, 8)
        pl.semaphore_signal(barrier, inc=1, device_id=(other // 2, lax.rem(other, 2)), device_id_type=MESH)

    y0_copy = pltpu.make_async_copy(y0_ref, state.at[0], y_sem)
    y0_copy.start()
    state[1] = jnp.zeros_like(state[1])
    y0_copy.wait()
    src[0, own_slot] = state[0].astype(jnp.bfloat16)
    pl.semaphore_wait(barrier, 7)
    for c in range(CHUNKS):
        send_own(0, c)

    def product(par, pair, c, cols):
        total = None
        for k in range(2):
            rows = pl.ds(pl.multiple_of((pair + k) * piece + OFFSETS[c], 128), WIDTHS[c])
            left = src[par, pair + k, :, pl.ds(OFFSETS[c], WIDTHS[c])]
            part = jnp.dot(left, tile[rows, cols], preferred_element_type=jnp.float32)
            total = part if total is None else total + part
        return total

    def apply_matrix(t, par, first, combine):
        for step, pair in enumerate((pair_first, pair_second)):
            for c in range(CHUNKS):
                passes_on = far if step == 0 else near
                takes = near if step == 0 else far

                @pl.when(passes_on)
                def _():
                    wait_slot(par, fwd_slot, c)
                    fwd_copy(par, c).start()
                    wait_slot(par, 2 * pair + 1 - fwd_slot, c)

                @pl.when(takes)
                def _():
                    if step == 0:
                        wait_slot(par, sib_slot, c)
                    else:
                        wait_slot(par, pair, c)
                        wait_slot(par, pair + 1, c)

                if first:
                    for k in range(2):
                        for half in range(2):
                            local_load(c, pair + k, half).wait()
                if step == 0 and c == 0:
                    acc[...] = product(par, pair, c, slice(None))
                elif step == 0 or c < CHUNKS - 1:
                    acc[...] += product(par, pair, c, slice(None))
                else:
                    for o in range(CHUNKS):
                        cols = pl.ds(OFFSETS[o], WIDTHS[o])
                        psend[:, cols] = acc[:, cols] + product(par, pair, c, cols)
                        partial_copy(par, o).start()
                    for o in range(CHUNKS):
                        cols = pl.ds(piece + OFFSETS[o], WIDTHS[o])
                        acc[:, cols] += product(par, pair, c, cols)
        for c in range(CHUNKS):
            fwd_copy(par, c).wait_send()
            wait_own_sends(par, c)
        for o in range(CHUNKS):
            partial_copy(par, o).wait_recv()
            cols = pl.ds(OFFSETS[o], WIDTHS[o])
            combine(o, acc[:, pl.ds(piece + OFFSETS[o], WIDTHS[o])] + prec[par, :, cols])
        for o in range(CHUNKS):
            partial_copy(par, o).wait_send()

    center = c_ref[0]
    half_width = e_ref[0]

    def advance(t, par, first):
        other = 1 - par

        def combine(o, image):
            cols = pl.ds(OFFSETS[o], WIDTHS[o])
            shifted = image - center * state[par, :, cols]
            if first:
                following = shifted / half_width
            else:
                following = 2.0 * shifted / half_width - state[other, :, cols]
            state[other, :, cols] = following
            src[other, own_slot, :, cols] = following.astype(jnp.bfloat16)
            send_own(other, o)

        apply_matrix(t, par, first, combine)

    advance(0, 0, True)

    def step(t, carry):
        advance(t, lax.rem(t, 2), False)
        return carry

    lax.fori_loop(1, DEGREE, step, 0)

    y_copy = pltpu.make_async_copy(state.at[0], y_out, y_sem)
    y_copy.start()

    gall[me] = jnp.zeros_like(gall[me])

    def gram_part(o, image):
        cols = pl.ds(OFFSETS[o], WIDTHS[o])
        gall[me] += lax.dot_general(src[0, own_slot, :, cols], image.astype(jnp.bfloat16), (((1,), (1,)), ((), ())), preferred_element_type=jnp.float32)

    apply_matrix(DEGREE, 0, False, gram_part)

    def gram_copy(d):
        other = lax.rem(me + d, 8)
        return remote(gall.at[me], gall.at[me], gsend_sem.at[d], grecv_sem.at[me], (other // 2, lax.rem(other, 2)))

    for d in range(1, 8):
        gram_copy(d).start()
    for d in range(1, 8):
        origin = lax.rem(me + d, 8)
        remote(gall.at[origin], gall.at[origin], gsend_sem.at[d], grecv_sem.at[origin], (chip, core)).wait_recv()
    total = gall[0]
    for d in range(1, 8):
        total = total + gall[d]
    g_out[...] = total / (8 * piece)
    for d in range(1, 8):
        gram_copy(d).wait_send()
    y_copy.wait()


def solution(mesh):
    def local_filter(mat_tile, y_start, center, half_width):
        piece, width = y_start.shape
        rows, cols = mat_tile.shape
        y_t, gram = pl.pallas_call(
            functools.partial(filter_kernel, piece, width),
            out_shape=(jax.ShapeDtypeStruct((width, piece), jnp.float32), jax.ShapeDtypeStruct((width, width), jnp.float32)),
            in_specs=[
                pl.BlockSpec(memory_space=pl.ANY),
                pl.BlockSpec(memory_space=pl.ANY),
                pl.BlockSpec(memory_space=pltpu.SMEM),
                pl.BlockSpec(memory_space=pltpu.SMEM),
            ],
            out_specs=(pl.BlockSpec(memory_space=pl.ANY), pl.BlockSpec(memory_space=pltpu.VMEM)),
            scratch_shapes=[
                pltpu.VMEM((rows, cols), jnp.bfloat16),
                pltpu.VMEM((2, 5, width, piece), jnp.bfloat16),
                pltpu.VMEM((2, width, piece), jnp.float32),
                pltpu.VMEM((width, cols), jnp.float32),
                pltpu.VMEM((width, piece), jnp.float32),
                pltpu.VMEM((2, width, piece), jnp.float32),
                pltpu.VMEM((8, width, width), jnp.float32),
                pltpu.SemaphoreType.DMA((4, CHUNKS, 2)),
                pltpu.SemaphoreType.DMA((2, 4, CHUNKS)),
                pltpu.SemaphoreType.DMA((3, CHUNKS)),
                pltpu.SemaphoreType.DMA((CHUNKS,)),
                pltpu.SemaphoreType.DMA((CHUNKS,)),
                pltpu.SemaphoreType.DMA((2, CHUNKS)),
                pltpu.SemaphoreType.DMA((8,)),
                pltpu.SemaphoreType.DMA((8,)),
                pltpu.SemaphoreType.DMA,
            ],
            compiler_params=pltpu.CompilerParams(collective_id=0, has_side_effects=True, vmem_limit_bytes=56 * 1024 * 1024),
            name="filter",
        )(mat_tile, y_start.T, center.reshape(1), half_width.reshape(1))
        return y_t.T, gram

    return jax.shard_map(local_filter, mesh=mesh, in_specs=(P("row", "col"), P(("col", "row"), None), P(), P()), out_specs=(P(("col", "row"), None), P()), check_vma=False)
```

```python
import functools

import jax
import jax.numpy as jnp
from jax import lax
from jax.experimental import pallas as pl
from jax.experimental.pallas import tpu as pltpu
from jax.sharding import PartitionSpec as P

DEGREE = 8
WIDTHS = (256, 512, 512, 128)
OFFSETS = (0, 256, 768, 1280)
CHUNKS = len(WIDTHS)
MESH = pl.DeviceIdType.MESH
EARLY, LATE = 0, 1


_held = []


def _push(rhs, staging_register, mxu_index, transpose=False):
    _held.append(rhs.T if transpose else rhs)


def _accl(acc, lhs, load_staged_rhs=None):
    acc[...] += jnp.dot(lhs, _held.pop(), preferred_element_type=jnp.float32)


def _pop(acc):
    value = acc[...]
    acc[...] = jnp.zeros_like(value)
    return value


def filter_kernel(piece, width, a_ref, y0_ref, c_ref, e_ref, y_out, g_out, tile, src, state, image, psend, prec, gall, tile_sem, recv_sem, send_sem, fwd_sem, psend_sem, prec_sem, gsend_sem, grecv_sem, y_sem):
    chip = lax.axis_index("col")
    core = lax.axis_index("row")
    me = chip * 2 + core
    sibling = 1 - core
    chip_bit = lax.rem(chip, 2)
    chip_x = chip + 1 - 2 * chip_bit
    chip_y = lax.rem(chip + 2, 4)
    group = chip // 2
    near_int = 1 - lax.abs(core - group)
    near = near_int == 1
    far = near_int == 0

    own_dest = 2 * chip_bit + core
    own_slot = near_int * own_dest + (1 - near_int) * 4
    pair_base = (2 * chip_bit, 2 * (1 - chip_bit))
    fwd_chip = near_int * chip_y + (1 - near_int) * chip_x

    def slot_of(step, kind):
        return pair_base[step] + (core if kind == LATE else sibling)

    def tile_load(step, kind, c, half):
        col = core if half else sibling
        rows = pl.ds(pl.multiple_of(slot_of(step, kind) * piece + OFFSETS[c], 128), WIDTHS[c])
        return pltpu.make_async_copy(
            a_ref.at[rows, pl.ds(pl.multiple_of(col * piece, 128), piece)],
            tile.at[rows, pl.ds(half * piece, piece)],
            tile_sem.at[step, kind, c, half],
        )

    def slot_view(par, slot, c):
        return src.at[par, slot, :, pl.ds(OFFSETS[c], WIDTHS[c])]

    def remote(src_view, dst_view, ssem, rsem, dev):
        return pltpu.make_async_remote_copy(src_ref=src_view, dst_ref=dst_view, send_sem=ssem, recv_sem=rsem, device_id=dev, device_id_type=MESH)

    def own_copy(par, c, d):
        dev = ((chip_x, group), (chip_y, group), (chip, group))[d]
        return remote(slot_view(par, own_slot, c), slot_view(par, own_dest, c), send_sem.at[d, c], recv_sem.at[par, own_dest, c], dev)

    def fwd_copy(par, step, kind, c):
        slot = slot_of(step, kind)
        return remote(slot_view(par, slot, c), slot_view(par, slot, c), fwd_sem.at[kind, c], recv_sem.at[par, slot, c], (fwd_chip, core))

    def wait_slot(par, slot, c):
        view = slot_view(par, slot, c)
        remote(view, view, fwd_sem.at[0, c], recv_sem.at[par, slot, c], (chip, core)).wait_recv()

    def partial_copy(par, o):
        cols = pl.ds(OFFSETS[o], WIDTHS[o])
        return remote(psend.at[:, cols], prec.at[par, :, cols], psend_sem.at[o], prec_sem.at[par, o], (chip, sibling))

    def send_own(par, c):
        own_copy(par, c, 0).start()
        own_copy(par, c, 1).start()

        @pl.when(far)
        def _():
            own_copy(par, c, 2).start()

    def wait_sends(par):
        for c in range(CHUNKS):
            own_copy(par, c, 0).wait_send()
            own_copy(par, c, 1).wait_send()

            @pl.when(far)
            def _():
                own_copy(par, c, 2).wait_send()

            for kind in (EARLY, LATE):

                @pl.when(near if (c + kind) % 2 == 0 else far)
                def _():
                    fwd_copy(par, 0, kind, c).wait_send()

    def arrive(par, step, kind, c):
        if step == 1:
            wait_slot(par, slot_of(1, kind), c)
            if (c + kind) % 2 == 0:

                @pl.when(near)
                def _():
                    fwd_copy(par, 1, kind, c).start()

            return

        if kind == EARLY:
            wait_slot(par, slot_of(0, kind), c)

        if kind == LATE or (c + kind) % 2 == 1:

            @pl.when(far)
            def _():
                if kind == LATE:
                    wait_slot(par, slot_of(0, kind), c)
                if (c + kind) % 2 == 1:
                    fwd_copy(par, 0, kind, c).start()

    y0_copy = pltpu.make_async_copy(y0_ref, state.at[0], y_sem)
    y0_copy.start()

    barrier = pltpu.get_barrier_semaphore()
    for d in range(1, 8):
        other = lax.rem(me + d, 8)
        pl.semaphore_signal(barrier, inc=1, device_id=(other // 2, lax.rem(other, 2)), device_id_type=MESH)

    for step in range(2):
        for kind in (EARLY, LATE):
            for c in range(CHUNKS):
                for half in range(2):
                    tile_load(step, kind, c, half).start()

    state[1] = jnp.zeros_like(state[1])
    y0_copy.wait()
    src[0, own_slot] = state[0].astype(jnp.bfloat16)
    pl.semaphore_wait(barrier, 7)
    for c in range(CHUNKS):
        send_own(0, c)
    center = c_ref[0]
    half_width = e_ref[0]

    def with_accumulators(accs0, accs1):
        for acc in accs0 + accs1:
            acc[...] = jnp.zeros_like(acc)

        def accumulate(par, halves, turn):
            lhs = jnp.concatenate([src[par, slot, :, pl.ds(off, 128)] for slot, off in halves], axis=1)
            for n in range(11):
                unit = n % 2 if n < 10 else turn % 2
                acc = (accs0, accs1)[unit][n // 2]
                parts = [tile[pl.ds(pl.multiple_of(slot * piece + off, 128), 128), pl.ds(256 * n, 256)] for slot, off in halves]
                reg = (n // 2 + turn) % 2
                _push(jnp.concatenate(parts, axis=0), staging_register=reg, mxu_index=unit)
                _accl(acc, lhs, load_staged_rhs=reg)

        def apply_matrix(par, first, combine):
            turn = 0
            for step in range(2):
                for kind in (EARLY, LATE):
                    slot = slot_of(step, kind)
                    for c in range(CHUNKS):
                        arrive(par, step, kind, c)
                        if first:
                            for half in range(2):
                                tile_load(step, kind, c, half).wait()
                        if c < CHUNKS - 1:
                            for k in range(WIDTHS[c] // 256):
                                off = OFFSETS[c] + 256 * k
                                accumulate(par, ((slot, off), (slot, off + 128)), turn)
                                turn += 1
                accumulate(par, ((slot_of(step, EARLY), OFFSETS[-1]), (slot_of(step, LATE), OFFSETS[-1])), turn)
                turn += 1
            for n in range(5):
                psend[:, pl.ds(256 * n, 256)] = _pop((accs0, accs1)[n % 2][n // 2])
            middle = _pop(accs1[2])
            psend[:, pl.ds(1280, 128)] = middle[:, :128]
            for o in range(CHUNKS):
                partial_copy(par, o).start()
            image[:, pl.ds(0, 128)] = middle[:, 128:]
            for n in range(6, 10):
                image[:, pl.ds(256 * n - piece, 256)] = _pop((accs0, accs1)[n % 2][n // 2])
            image[:, pl.ds(1152, 256)] = _pop(accs0[5]) + _pop(accs1[5])
            wait_sends(par)
            for o in range(CHUNKS):
                partial_copy(par, o).wait_recv()
                cols = pl.ds(OFFSETS[o], WIDTHS[o])
                combine(o, image[:, cols] + prec[par, :, cols])
            for o in range(CHUNKS):
                partial_copy(par, o).wait_send()

        def advance(par, first):
            other = 1 - par

            def combine(o, total):
                cols = pl.ds(OFFSETS[o], WIDTHS[o])
                shifted = total - center * state[par, :, cols]
                if first:
                    following = shifted / half_width
                else:
                    following = 2.0 * shifted / half_width - state[other, :, cols]
                state[other, :, cols] = following
                src[other, own_slot, :, cols] = following.astype(jnp.bfloat16)
                send_own(other, o)

            apply_matrix(par, first, combine)

        advance(0, True)

        def step(t, carry):
            advance(lax.rem(t, 2), False)
            return carry

        lax.fori_loop(1, DEGREE, step, 0)

        y_copy = pltpu.make_async_copy(state.at[0], y_out, y_sem)
        y_copy.start()

        def gram_part(o, total):
            low = total.astype(jnp.bfloat16)
            for k in range(max(WIDTHS[o] // 256, 1)):
                size = min(WIDTHS[o], 256)
                left = src[0, own_slot, :, pl.ds(OFFSETS[o] + 256 * k, size)]
                right = low[:, 256 * k : 256 * k + size]
                if size < 256:
                    left = jnp.concatenate([left, jnp.zeros_like(left)], axis=1)
                    right = jnp.concatenate([right, jnp.zeros_like(right)], axis=1)
                right = jnp.concatenate([right, jnp.zeros((256 - width, 256), jnp.bfloat16)], axis=0)
                unit = (o + k) % 2
                _push(right, staging_register=0, mxu_index=unit, transpose=True)
                _accl((accs0, accs1)[unit][0], left, load_staged_rhs=0)

        apply_matrix(0, False, gram_part)
        gall[me] = (_pop(accs0[0]) + _pop(accs1[0]))[:, :width]

        def gram_copy(d):
            other = lax.rem(me + d, 8)
            return remote(gall.at[me], gall.at[me], gsend_sem.at[d], grecv_sem.at[me], (other // 2, lax.rem(other, 2)))

        for d in range(1, 8):
            gram_copy(d).start()
        for d in range(1, 8):
            origin = lax.rem(me + d, 8)
            remote(gall.at[origin], gall.at[origin], gsend_sem.at[d], grecv_sem.at[origin], (chip, core)).wait_recv()
        total = gall[0]
        for d in range(1, 8):
            total = total + gall[d]
        g_out[...] = total / (8 * piece)
        for d in range(1, 8):
            gram_copy(d).wait_send()
        y_copy.wait()

    accs = [tuple(pltpu.VMEM((width, 256), jnp.float32) for _ in range(6)) for unit in range(2)]
    pl.run_scoped(with_accumulators, *accs)


def solution(mesh):
    def local_filter(mat_tile, y_start, center, half_width):
        piece, width = y_start.shape
        rows, cols = mat_tile.shape
        y_t, gram = pl.pallas_call(
            functools.partial(filter_kernel, piece, width),
            out_shape=(jax.ShapeDtypeStruct((width, piece), jnp.float32), jax.ShapeDtypeStruct((width, width), jnp.float32)),
            in_specs=[pl.BlockSpec(memory_space=pl.ANY)] * 2 + [pl.BlockSpec(memory_space=pltpu.SMEM)] * 2,
            out_specs=(pl.BlockSpec(memory_space=pl.ANY), pl.BlockSpec(memory_space=pltpu.VMEM)),
            scratch_shapes=[
                pltpu.VMEM((rows, cols), jnp.bfloat16),
                pltpu.VMEM((2, 5, width, piece), jnp.bfloat16),
                pltpu.VMEM((2, width, piece), jnp.float32),
                pltpu.VMEM((width, piece), jnp.float32),
                pltpu.VMEM((width, piece), jnp.float32),
                pltpu.VMEM((2, width, piece), jnp.float32),
                pltpu.VMEM((8, width, width), jnp.float32),
                pltpu.SemaphoreType.DMA((2, 2, CHUNKS, 2)),
                pltpu.SemaphoreType.DMA((2, 4, CHUNKS)),
                pltpu.SemaphoreType.DMA((3, CHUNKS)),
                pltpu.SemaphoreType.DMA((2, CHUNKS)),
                pltpu.SemaphoreType.DMA((CHUNKS,)),
                pltpu.SemaphoreType.DMA((2, CHUNKS)),
                pltpu.SemaphoreType.DMA((8,)),
                pltpu.SemaphoreType.DMA((8,)),
                pltpu.SemaphoreType.DMA,
            ],
            compiler_params=pltpu.CompilerParams(collective_id=0, has_side_effects=True, vmem_limit_bytes=56 * 1024 * 1024),
            name="filter",
        )(mat_tile, y_start.T, center.reshape(1), half_width.reshape(1))
        return y_t.T, gram

    return jax.shard_map(local_filter, mesh=mesh, in_specs=(P("row", "col"), P(("col", "row"), None), P(), P()), out_specs=(P(("col", "row"), None), P()), check_vma=False)
```

```python
import functools

import jax
import jax.numpy as jnp
from jax import lax
from jax.experimental import pallas as pl
from jax.experimental.pallas import tpu as pltpu
from jax.sharding import PartitionSpec as P

DEGREE = 8
WIDTHS = (256, 512, 512, 128)
OFFSETS = (0, 256, 768, 1280)
CHUNKS = len(WIDTHS)
BLOCKS = ((0, 1), (2, 3))
FINAL_BLOCKS = ((0, 1), (2,), (3,))
MESH = pl.DeviceIdType.MESH
EARLY, LATE = 0, 1


def filter_kernel(piece, width, a_ref, y0_ref, c_ref, e_ref, y_out, g_out, tile, src, state, acc, psend, prec, gall, tile_sem, recv_sem, send_sem, fwd_sem, psend_sem, prec_sem, gsend_sem, grecv_sem, y_sem):
    chip = lax.axis_index("col")
    core = lax.axis_index("row")
    me = chip * 2 + core
    sibling = 1 - core
    chip_bit = lax.rem(chip, 2)
    chip_x = chip + 1 - 2 * chip_bit
    chip_y = lax.rem(chip + 2, 4)
    group = chip // 2
    near_int = 1 - lax.abs(core - group)
    near = near_int == 1
    far = near_int == 0

    own_dest = 2 * chip_bit + core
    own_slot = near_int * own_dest + (1 - near_int) * 4
    pair_base = (2 * chip_bit, 2 * (1 - chip_bit))
    fwd_chip = near_int * chip_y + (1 - near_int) * chip_x

    def slot_of(step, kind):
        return pair_base[step] + (core if kind == LATE else sibling)

    def tile_load(step, kind, c, half):
        col = core if half else sibling
        rows = pl.ds(pl.multiple_of(slot_of(step, kind) * piece + OFFSETS[c], 128), WIDTHS[c])
        return pltpu.make_async_copy(
            a_ref.at[rows, pl.ds(pl.multiple_of(col * piece, 128), piece)],
            tile.at[rows, pl.ds(half * piece, piece)],
            tile_sem.at[step, kind, c, half],
        )

    def slot_view(par, slot, c):
        return src.at[par, slot, :, pl.ds(OFFSETS[c], WIDTHS[c])]

    def remote(src_view, dst_view, ssem, rsem, dev):
        return pltpu.make_async_remote_copy(src_ref=src_view, dst_ref=dst_view, send_sem=ssem, recv_sem=rsem, device_id=dev, device_id_type=MESH)

    def own_copy(par, c, d):
        dev = ((chip_x, group), (chip_y, group), (chip, group))[d]
        return remote(slot_view(par, own_slot, c), slot_view(par, own_dest, c), send_sem.at[d, c], recv_sem.at[par, own_dest, c], dev)

    def fwd_copy(par, step, kind, c):
        slot = slot_of(step, kind)
        return remote(slot_view(par, slot, c), slot_view(par, slot, c), fwd_sem.at[kind, c], recv_sem.at[par, slot, c], (fwd_chip, core))

    def wait_slot(par, slot, c):
        view = slot_view(par, slot, c)
        remote(view, view, fwd_sem.at[0, c], recv_sem.at[par, slot, c], (chip, core)).wait_recv()

    def partial_copy(par, o):
        cols = pl.ds(OFFSETS[o], WIDTHS[o])
        return remote(psend.at[:, cols], prec.at[par, :, cols], psend_sem.at[o], prec_sem.at[par, o], (chip, sibling))

    def send_own(par, c):
        own_copy(par, c, 0).start()
        own_copy(par, c, 1).start()

        @pl.when(far)
        def _():
            own_copy(par, c, 2).start()

    def wait_sends(par):
        for c in range(CHUNKS):
            own_copy(par, c, 0).wait_send()
            own_copy(par, c, 1).wait_send()

            @pl.when(far)
            def _():
                own_copy(par, c, 2).wait_send()

            for kind in (EARLY, LATE):

                @pl.when(near if (c + kind) % 2 == 0 else far)
                def _():
                    fwd_copy(par, 0, kind, c).wait_send()

    def arrive(par, step, kind, c):
        if step == 1:
            wait_slot(par, slot_of(1, kind), c)
            if (c + kind) % 2 == 0:

                @pl.when(near)
                def _():
                    fwd_copy(par, 1, kind, c).start()

            return

        if kind == EARLY:
            wait_slot(par, slot_of(0, kind), c)

        if kind == LATE or (c + kind) % 2 == 1:

            @pl.when(far)
            def _():
                if kind == LATE:
                    wait_slot(par, slot_of(0, kind), c)
                if (c + kind) % 2 == 1:
                    fwd_copy(par, 0, kind, c).start()

    y0_copy = pltpu.make_async_copy(y0_ref, state.at[0], y_sem)
    y0_copy.start()

    barrier = pltpu.get_barrier_semaphore()
    for d in range(1, 8):
        other = lax.rem(me + d, 8)
        pl.semaphore_signal(barrier, inc=1, device_id=(other // 2, lax.rem(other, 2)), device_id_type=MESH)

    for step in range(2):
        for kind in (EARLY, LATE):
            for c in range(CHUNKS):
                for half in range(2):
                    tile_load(step, kind, c, half).start()

    state[1] = jnp.zeros_like(state[1])
    acc[...] = jnp.zeros_like(acc)
    y0_copy.wait()
    src[0, own_slot] = state[0].astype(jnp.bfloat16)
    pl.semaphore_wait(barrier, 7)
    for c in range(CHUNKS):
        send_own(0, c)
    center = c_ref[()]
    half_width = e_ref[()]

    def product(par, slot, off, size, cols):
        rows = pl.ds(pl.multiple_of(slot * piece + off, 128), size)
        return jnp.dot(src[par, slot, :, pl.ds(off, size)], tile[rows, cols], preferred_element_type=jnp.float32)

    def apply_matrix(par, first, combine):
        for step in range(2):
            for kind in (EARLY, LATE):
                slot = slot_of(step, kind)
                final = step == 1 and kind == LATE
                for block in FINAL_BLOCKS if final else BLOCKS:
                    for c in block:
                        arrive(par, step, kind, c)
                        if first:
                            for half in range(2):
                                tile_load(step, kind, c, half).wait()
                    off, size = OFFSETS[block[0]], sum(WIDTHS[c] for c in block)
                    if final and block[0] == CHUNKS - 1:
                        psend[...] = acc[:, :piece] + product(par, slot, off, size, pl.ds(0, piece))
                        acc[:, piece:] += product(par, slot, off, size, pl.ds(piece, piece))
                    else:
                        acc[...] += product(par, slot, off, size, slice(None))
        for o in range(CHUNKS):
            partial_copy(par, o).start()
        wait_sends(par)
        for o in range(CHUNKS):
            partial_copy(par, o).wait_recv()
            combine(o, acc[:, pl.ds(piece + OFFSETS[o], WIDTHS[o])] + prec[par, :, pl.ds(OFFSETS[o], WIDTHS[o])])
        acc[...] = jnp.zeros_like(acc)
        for o in range(CHUNKS):
            partial_copy(par, o).wait_send()

    def advance(par, first):
        other = 1 - par

        def combine(o, total):
            cols = pl.ds(OFFSETS[o], WIDTHS[o])
            shifted = total - center * state[par, :, cols]
            if first:
                following = shifted / half_width
            else:
                following = 2.0 * shifted / half_width - state[other, :, cols]
            state[other, :, cols] = following
            src[other, own_slot, :, cols] = following.astype(jnp.bfloat16)
            send_own(other, o)

        apply_matrix(par, first, combine)

    advance(0, True)

    def step(t, carry):
        advance(lax.rem(t, 2), False)
        return carry

    lax.fori_loop(1, DEGREE, step, 0)

    y_out[...] = state[0]
    gall[me] = jnp.zeros_like(gall[me])

    def gram_part(o, total):
        cols = pl.ds(OFFSETS[o], WIDTHS[o])
        gall[me] += lax.dot_general(src[0, own_slot, :, cols], total.astype(jnp.bfloat16), (((1,), (1,)), ((), ())), preferred_element_type=jnp.float32)

    apply_matrix(0, False, gram_part)

    def gram_copy(d):
        other = lax.rem(me + d, 8)
        return remote(gall.at[me], gall.at[me], gsend_sem.at[d], grecv_sem.at[me], (other // 2, lax.rem(other, 2)))

    for d in range(1, 8):
        gram_copy(d).start()
    for d in range(1, 8):
        origin = lax.rem(me + d, 8)
        remote(gall.at[origin], gall.at[origin], gsend_sem.at[d], grecv_sem.at[origin], (chip, core)).wait_recv()
    total = gall[0]
    for d in range(1, 8):
        total = total + gall[d]
    g_out[...] = total / (8 * piece)
    for d in range(1, 8):
        gram_copy(d).wait_send()


def solution(mesh):
    def local_filter(mat_tile, y_start, center, half_width):
        piece, width = y_start.shape
        rows, cols = mat_tile.shape
        y_t, gram = pl.pallas_call(
            functools.partial(filter_kernel, piece, width),
            out_shape=(pltpu.VMEM((width, piece), jnp.float32), pltpu.VMEM((width, width), jnp.float32)),
            in_specs=[pl.BlockSpec(memory_space=pl.ANY)] * 2 + [pl.BlockSpec(memory_space=pltpu.SMEM)] * 2,
            out_specs=(pl.BlockSpec(memory_space=pltpu.VMEM),) * 2,
            scratch_shapes=[
                pltpu.VMEM((rows, cols), jnp.bfloat16),
                pltpu.VMEM((2, 5, width, piece), jnp.bfloat16),
                pltpu.VMEM((2, width, piece), jnp.float32),
                pltpu.VMEM((width, cols), jnp.float32),
                pltpu.VMEM((width, piece), jnp.float32),
                pltpu.VMEM((2, width, piece), jnp.float32),
                pltpu.VMEM((8, width, width), jnp.float32),
                pltpu.SemaphoreType.DMA((2, 2, CHUNKS, 2)),
                pltpu.SemaphoreType.DMA((2, 4, CHUNKS)),
                pltpu.SemaphoreType.DMA((3, CHUNKS)),
                pltpu.SemaphoreType.DMA((2, CHUNKS)),
                pltpu.SemaphoreType.DMA((CHUNKS,)),
                pltpu.SemaphoreType.DMA((2, CHUNKS)),
                pltpu.SemaphoreType.DMA((8,)),
                pltpu.SemaphoreType.DMA((8,)),
                pltpu.SemaphoreType.DMA,
            ],
            compiler_params=pltpu.CompilerParams(collective_id=0, has_side_effects=True, vmem_limit_bytes=56 * 1024 * 1024),
            name="filter",
        )(mat_tile, y_start.T, center, half_width)
        return y_t.T, gram

    return jax.shard_map(local_filter, mesh=mesh, in_specs=(P("row", "col"), P(("col", "row"), None), P(), P()), out_specs=(P(("col", "row"), None), P()), check_vma=False)
```

```python
import functools

import jax
import jax.numpy as jnp
from jax import lax
from jax.experimental import pallas as pl
from jax.experimental.pallas import tpu as pltpu
from jax.sharding import PartitionSpec as P

DEGREE = 8
WIDTHS = (256, 256, 256, 256, 256, 128)
OFFSETS = (0, 256, 512, 768, 1024, 1280)
CHUNKS = len(WIDTHS)
MESH = pl.DeviceIdType.MESH
EARLY, LATE = 0, 1
BLOCKS = (
    (((EARLY, 0, 0),), ((EARLY, 1, 2),), ((LATE, 0, 0), (EARLY, 3, 3)), ((LATE, 1, 1), (EARLY, 4, 5)), ((LATE, 2, 3),), ((LATE, 4, 5),)),
    (((EARLY, 0, 1),), ((EARLY, 2, 3), (LATE, 0, 0)), ((LATE, 1, 1), (EARLY, 4, 5), (LATE, 2, 2)), ((LATE, 3, 5),)),
)


def filter_kernel(piece, width, a_ref, y0_ref, c_ref, e_ref, y_out, g_out, tile, src, state, acc, prec, gall, image, tile_sem, recv_sem, send_sem, fwd_sem, psend_sem, prec_sem, gsend_sem, grecv_sem, y_sem):
    chip = lax.axis_index("col")
    core = lax.axis_index("row")
    me = chip * 2 + core
    sibling = 1 - core
    chip_bit = lax.rem(chip, 2)
    chip_x = chip + 1 - 2 * chip_bit
    chip_y = lax.rem(chip + 2, 4)
    group = chip // 2
    near_int = 1 - lax.abs(core - group)
    near = near_int == 1
    far = near_int == 0

    own_dest = 2 * chip_bit + core
    own_slot = near_int * own_dest + (1 - near_int) * 4
    pair_base = (2 * chip_bit, 2 * (1 - chip_bit))
    fwd_chip = near_int * chip_y + (1 - near_int) * chip_x

    def slot_of(step, kind):
        return pair_base[step] + (core if kind == LATE else sibling)

    def tile_load(step, kind, c, half):
        col = core if half else sibling
        rows = pl.ds(pl.multiple_of(slot_of(step, kind) * piece + OFFSETS[c], 128), WIDTHS[c])
        return pltpu.make_async_copy(
            a_ref.at[rows, pl.ds(pl.multiple_of(col * piece, 128), piece)],
            tile.at[rows, pl.ds(half * piece, piece)],
            tile_sem.at[step, kind, c, half],
        )

    def slot_view(par, slot, c):
        return src.at[par, slot, :, pl.ds(OFFSETS[c], WIDTHS[c])]

    def remote(src_view, dst_view, ssem, rsem, dev):
        return pltpu.make_async_remote_copy(src_ref=src_view, dst_ref=dst_view, send_sem=ssem, recv_sem=rsem, device_id=dev, device_id_type=MESH)

    def own_copy(par, c, d):
        dev = ((chip_x, group), (chip_y, group), (chip, group))[d]
        return remote(slot_view(par, own_slot, c), slot_view(par, own_dest, c), send_sem.at[d, c], recv_sem.at[par, own_dest, c], dev)

    def fwd_copy(par, step, kind, c):
        slot = slot_of(step, kind)
        return remote(slot_view(par, slot, c), slot_view(par, slot, c), fwd_sem.at[kind, c], recv_sem.at[par, slot, c], (fwd_chip, core))

    def wait_slot(par, slot, c):
        view = slot_view(par, slot, c)
        remote(view, view, fwd_sem.at[0, c], recv_sem.at[par, slot, c], (chip, core)).wait_recv()

    def partial_copy(par, o):
        cols = pl.ds(OFFSETS[o], WIDTHS[o])
        return remote(acc.at[:, cols], prec.at[par, :, cols], psend_sem.at[o], prec_sem.at[par, o], (chip, sibling))

    def send_own(par, c):
        own_copy(par, c, 0).start()
        own_copy(par, c, 1).start()

        @pl.when(far)
        def _():
            own_copy(par, c, 2).start()

    def wait_sends(par):
        for c in range(CHUNKS):
            own_copy(par, c, 0).wait_send()
            own_copy(par, c, 1).wait_send()

            @pl.when(far)
            def _():
                own_copy(par, c, 2).wait_send()

            for kind in (EARLY, LATE):

                @pl.when(near if (c + kind) % 2 == 0 else far)
                def _():
                    fwd_copy(par, 0, kind, c).wait_send()

    def arrive(par, step, kind, c):
        if step == 1:
            wait_slot(par, slot_of(1, kind), c)
            if (c + kind) % 2 == 0:

                @pl.when(near)
                def _():
                    fwd_copy(par, 1, kind, c).start()

            return

        if kind == EARLY:
            wait_slot(par, slot_of(0, kind), c)

        if kind == LATE or (c + kind) % 2 == 1:

            @pl.when(far)
            def _():
                if kind == LATE:
                    wait_slot(par, slot_of(0, kind), c)
                if (c + kind) % 2 == 1:
                    fwd_copy(par, 0, kind, c).start()

    y0_copy = pltpu.make_async_copy(y0_ref, state.at[0], y_sem)
    y0_copy.start()

    barrier = pltpu.get_barrier_semaphore()
    for d in range(1, 8):
        other = lax.rem(me + d, 8)
        pl.semaphore_signal(barrier, inc=1, device_id=(other // 2, lax.rem(other, 2)), device_id_type=MESH)

    for step in range(2):
        for kind in (EARLY, LATE):
            for c in range(CHUNKS):
                for half in range(2):
                    tile_load(step, kind, c, half).start()

    state[1] = jnp.zeros_like(state[1])
    y0_copy.wait()
    src[0, own_slot] = state[0].astype(jnp.bfloat16)
    pl.semaphore_wait(barrier, 7)
    for c in range(CHUNKS):
        send_own(0, c)
    center = c_ref[()]
    half_width = e_ref[()]

    def product(par, slot, off, size, cols):
        rows = pl.ds(pl.multiple_of(slot * piece + off, 128), size)
        return jnp.dot(src[par, slot, :, pl.ds(off, size)], tile[rows, cols], preferred_element_type=jnp.float32)

    def apply_matrix(par, first, combine):
        for step in range(2):
            for index, block in enumerate(BLOCKS[step]):
                for kind, low, high in block:
                    for c in range(low, high + 1):
                        arrive(par, step, kind, c)
                        if first:
                            for half in range(2):
                                tile_load(step, kind, c, half).wait()

                def total(cols):
                    parts = [product(par, slot_of(step, kind), OFFSETS[low], OFFSETS[high] + WIDTHS[high] - OFFSETS[low], cols) for kind, low, high in block]
                    return sum(parts[1:], parts[0])

                if step == 0 and index == 0:
                    acc[...] = total(slice(None))
                else:
                    acc[...] += total(slice(None))
        for o in range(CHUNKS):
            partial_copy(par, o).start()
        wait_sends(par)
        for o in range(CHUNKS):
            partial_copy(par, o).wait_recv()
            combine(o, acc[:, pl.ds(piece + OFFSETS[o], WIDTHS[o])] + prec[par, :, pl.ds(OFFSETS[o], WIDTHS[o])])
        for o in range(CHUNKS):
            partial_copy(par, o).wait_send()

    def advance(par, first):
        other = 1 - par

        def combine(o, total):
            cols = pl.ds(OFFSETS[o], WIDTHS[o])
            shifted = total - center * state[par, :, cols]
            if first:
                following = shifted / half_width
            else:
                following = 2.0 * shifted / half_width - state[other, :, cols]
            state[other, :, cols] = following
            src[other, own_slot, :, cols] = following.astype(jnp.bfloat16)
            send_own(other, o)

        apply_matrix(par, first, combine)

    advance(0, True)

    def step(t, carry):
        advance(lax.rem(t, 2), False)
        return carry

    lax.fori_loop(1, DEGREE, step, 0)

    y_out[...] = state[0]

    def gram_part(o, total):
        image[:, pl.ds(OFFSETS[o], WIDTHS[o])] = total.astype(jnp.bfloat16)

    apply_matrix(0, False, gram_part)
    gram_part_sum = lax.dot_general(src[0, own_slot], image[...], (((1,), (1,)), ((), ())), preferred_element_type=jnp.float32)
    half = width // 2
    gall[me] = jnp.concatenate([gram_part_sum[:half], gram_part_sum[half:]], axis=1)

    def gram_copy(d):
        other = lax.rem(me + d, 8)
        return remote(gall.at[me], gall.at[me], gsend_sem.at[d], grecv_sem.at[me], (other // 2, lax.rem(other, 2)))

    for d in range(1, 8):
        gram_copy(d).start()
    for d in range(1, 8):
        origin = lax.rem(me + d, 8)
        remote(gall.at[origin], gall.at[origin], gsend_sem.at[d], grecv_sem.at[origin], (chip, core)).wait_recv()
    total = gall[0]
    for d in range(1, 8):
        total = total + gall[d]
    total = total / (8 * piece)
    g_out[:half] = total[:, :width]
    g_out[half:] = total[:, width:]
    for d in range(1, 8):
        gram_copy(d).wait_send()


def solution(mesh):
    def local_filter(mat_tile, y_start, center, half_width):
        piece, width = y_start.shape
        rows, cols = mat_tile.shape
        y_t, gram = pl.pallas_call(
            functools.partial(filter_kernel, piece, width),
            out_shape=(pltpu.VMEM((width, piece), jnp.float32), pltpu.VMEM((width, width), jnp.float32)),
            in_specs=[pl.BlockSpec(memory_space=pl.ANY)] * 2 + [pl.BlockSpec(memory_space=pltpu.SMEM)] * 2,
            out_specs=(pl.BlockSpec(memory_space=pltpu.VMEM),) * 2,
            scratch_shapes=[
                pltpu.VMEM((rows, cols), jnp.bfloat16),
                pltpu.VMEM((2, 5, width, piece), jnp.bfloat16),
                pltpu.VMEM((2, width, piece), jnp.float32),
                pltpu.VMEM((width, cols), jnp.float32),
                pltpu.VMEM((2, width, piece), jnp.float32),
                pltpu.VMEM((8, width // 2, 2 * width), jnp.float32),
                pltpu.VMEM((width, piece), jnp.bfloat16),
                pltpu.SemaphoreType.DMA((2, 2, CHUNKS, 2)),
                pltpu.SemaphoreType.DMA((2, 4, CHUNKS)),
                pltpu.SemaphoreType.DMA((3, CHUNKS)),
                pltpu.SemaphoreType.DMA((2, CHUNKS)),
                pltpu.SemaphoreType.DMA((CHUNKS,)),
                pltpu.SemaphoreType.DMA((2, CHUNKS)),
                pltpu.SemaphoreType.DMA((8,)),
                pltpu.SemaphoreType.DMA((8,)),
                pltpu.SemaphoreType.DMA,
            ],
            compiler_params=pltpu.CompilerParams(collective_id=0, has_side_effects=True, vmem_limit_bytes=56 * 1024 * 1024),
            name="filter",
        )(mat_tile, y_start.T, center, half_width)
        return y_t.T, gram

    return jax.shard_map(local_filter, mesh=mesh, in_specs=(P("row", "col"), P(("col", "row"), None), P(), P()), out_specs=(P(("col", "row"), None), P()), check_vma=False)
```

```python
import functools

import jax
import jax.numpy as jnp
from jax import lax
from jax.experimental import pallas as pl
from jax.experimental.pallas import tpu as pltpu
from jax.sharding import PartitionSpec as P

DEGREE = 8
WIDTHS = (256, 256, 256, 256, 256, 128)
OFFSETS = (0, 256, 512, 768, 1024, 1280)
CHUNKS = len(WIDTHS)
MESH = pl.DeviceIdType.MESH
EARLY, LATE = 0, 1
BLOCKS = (
    (((EARLY, 0, 0),), ((EARLY, 1, 2),), ((EARLY, 3, 3), (LATE, 0, 0)), ((LATE, 1, 1), (EARLY, 4, 4)), ((EARLY, 5, 5), (LATE, 2, 3)), ((LATE, 4, 5),)),
    (((EARLY, 1, 1), (EARLY, 3, 3), (LATE, 0, 0)), ((EARLY, 5, 5), (LATE, 2, 2), (LATE, 4, 4)), ((EARLY, 0, 0), (EARLY, 2, 2), (LATE, 1, 1)), ((EARLY, 4, 4), (LATE, 3, 3)), ((LATE, 5, 5),)),
)
PASSED = (((EARLY, 0), (EARLY, 2), (LATE, 1)), ((EARLY, 4), (LATE, 3)), ((LATE, 5),), (), ())


def filter_kernel(piece, width, a_ref, y0_ref, c_ref, e_ref, y_out, g_out, tile, src, state, acc, prec, gall, image, tile_sem, recv_sem, send_sem, fwd_sem, psend_sem, prec_sem, gsend_sem, grecv_sem, y_sem):
    chip = lax.axis_index("col")
    core = lax.axis_index("row")
    me = chip * 2 + core
    sibling = 1 - core
    chip_bit = lax.rem(chip, 2)
    chip_x = chip + 1 - 2 * chip_bit
    chip_y = lax.rem(chip + 2, 4)
    group = chip // 2
    near_int = 1 - lax.abs(core - group)
    near = near_int == 1
    far = near_int == 0

    own_dest = 2 * chip_bit + core
    own_slot = near_int * own_dest + (1 - near_int) * 4
    pair_base = (2 * chip_bit, 2 * (1 - chip_bit))
    fwd_chip = near_int * chip_y + (1 - near_int) * chip_x

    def slot_of(step, kind):
        return pair_base[step] + (core if kind == LATE else sibling)

    def tile_load(step, kind, c, half):
        col = core if half else sibling
        rows = pl.ds(pl.multiple_of(slot_of(step, kind) * piece + OFFSETS[c], 128), WIDTHS[c])
        return pltpu.make_async_copy(
            a_ref.at[rows, pl.ds(pl.multiple_of(col * piece, 128), piece)],
            tile.at[rows, pl.ds(half * piece, piece)],
            tile_sem.at[step, kind, c, half],
        )

    def slot_view(par, slot, c):
        return src.at[par, slot, :, pl.ds(OFFSETS[c], WIDTHS[c])]

    def remote(src_view, dst_view, ssem, rsem, dev):
        return pltpu.make_async_remote_copy(src_ref=src_view, dst_ref=dst_view, send_sem=ssem, recv_sem=rsem, device_id=dev, device_id_type=MESH)

    def own_copy(par, c, d):
        dev = ((chip_x, group), (chip_y, group), (chip, group))[d]
        return remote(slot_view(par, own_slot, c), slot_view(par, own_dest, c), send_sem.at[d, c], recv_sem.at[par, own_dest, c], dev)

    def fwd_copy(par, step, kind, c):
        slot = slot_of(step, kind)
        return remote(slot_view(par, slot, c), slot_view(par, slot, c), fwd_sem.at[kind, c], recv_sem.at[par, slot, c], (fwd_chip, core))

    def wait_slot(par, slot, c):
        view = slot_view(par, slot, c)
        remote(view, view, fwd_sem.at[0, c], recv_sem.at[par, slot, c], (chip, core)).wait_recv()

    def partial_copy(par, o):
        cols = pl.ds(OFFSETS[o], WIDTHS[o])
        return remote(acc.at[:, cols], prec.at[par, :, cols], psend_sem.at[o], prec_sem.at[par, o], (chip, sibling))

    def send_own(par, c):
        own_copy(par, c, 0).start()
        own_copy(par, c, 1).start()

        @pl.when(far)
        def _():
            own_copy(par, c, 2).start()

    def wait_sends(par):
        for c in range(CHUNKS):
            own_copy(par, c, 0).wait_send()
            own_copy(par, c, 1).wait_send()

            @pl.when(far)
            def _():
                own_copy(par, c, 2).wait_send()

            for kind in (EARLY, LATE):

                @pl.when(near if (c + kind) % 2 == 0 else far)
                def _():
                    fwd_copy(par, 0, kind, c).wait_send()

    def arrive(par, step, kind, c):
        if step == 1:
            if (c + kind) % 2 == 0:

                @pl.when(far)
                def _():
                    wait_slot(par, slot_of(1, kind), c)

            else:
                wait_slot(par, slot_of(1, kind), c)
            return

        if kind == EARLY:
            wait_slot(par, slot_of(0, kind), c)

        if kind == LATE or (c + kind) % 2 == 1:

            @pl.when(far)
            def _():
                if kind == LATE:
                    wait_slot(par, slot_of(0, kind), c)
                if (c + kind) % 2 == 1:
                    fwd_copy(par, 0, kind, c).start()

    y0_copy = pltpu.make_async_copy(y0_ref, state.at[0], y_sem)
    y0_copy.start()

    padding = pl.ds(2 * piece, acc.shape[1] - 2 * piece)
    tile[:, padding] = jnp.zeros_like(tile[:, padding])
    barrier = pltpu.get_barrier_semaphore()
    for d in range(1, 8):
        other = lax.rem(me + d, 8)
        pl.semaphore_signal(barrier, inc=1, device_id=(other // 2, lax.rem(other, 2)), device_id_type=MESH)

    for step in range(2):
        for kind in (EARLY, LATE):
            for c in range(CHUNKS):
                for half in range(2):
                    tile_load(step, kind, c, half).start()

    state[1] = jnp.zeros_like(state[1])
    y0_copy.wait()
    src[0, own_slot] = state[0].astype(jnp.bfloat16)
    pl.semaphore_wait(barrier, 7)
    for c in range(CHUNKS):
        send_own(0, c)
    center = c_ref[()]
    half_width = e_ref[()]

    def product(par, slot, off, size, cols):
        rows = pl.ds(pl.multiple_of(slot * piece + off, 128), size)
        return jnp.dot(src[par, slot, :, pl.ds(off, size)], tile[rows, cols], preferred_element_type=jnp.float32)

    def apply_matrix(par, first, combine):
        for step in range(2):
            for index, block in enumerate(BLOCKS[step]):
                if step == 1 and PASSED[index]:

                    @pl.when(near)
                    def _():
                        for kind, c in PASSED[index]:
                            wait_slot(par, slot_of(1, kind), c)
                            fwd_copy(par, 1, kind, c).start()

                for kind, low, high in block:
                    for c in range(low, high + 1):
                        arrive(par, step, kind, c)
                        if first:
                            for half in range(2):
                                tile_load(step, kind, c, half).wait()

                def total(cols):
                    parts = [product(par, slot_of(step, kind), OFFSETS[low], OFFSETS[high] + WIDTHS[high] - OFFSETS[low], cols) for kind, low, high in block]
                    return sum(parts[1:], parts[0])

                if step == 0 and index == 0:
                    acc[...] = total(slice(None))
                else:
                    acc[...] += total(slice(None))
        for o in range(CHUNKS):
            partial_copy(par, o).start()
        wait_sends(par)
        for o in range(CHUNKS):
            partial_copy(par, o).wait_recv()
            combine(o, acc[:, pl.ds(piece + OFFSETS[o], WIDTHS[o])] + prec[par, :, pl.ds(OFFSETS[o], WIDTHS[o])])
        for o in range(CHUNKS):
            partial_copy(par, o).wait_send()

    def advance(par, first):
        other = 1 - par

        def combine(o, total):
            cols = pl.ds(OFFSETS[o], WIDTHS[o])
            shifted = total - center * state[par, :, cols]
            if first:
                following = shifted / half_width
            else:
                following = 2.0 * shifted / half_width - state[other, :, cols]
            state[other, :, cols] = following
            src[other, own_slot, :, cols] = following.astype(jnp.bfloat16)
            send_own(other, o)

        apply_matrix(par, first, combine)

    advance(0, True)

    def step(t, carry):
        advance(lax.rem(t, 2), False)
        return carry

    lax.fori_loop(1, DEGREE, step, 0)

    y_out[...] = state[0]

    def gram_part(o, total):
        image[:, pl.ds(OFFSETS[o], WIDTHS[o])] = total.astype(jnp.bfloat16)

    apply_matrix(0, False, gram_part)
    gram_part_sum = lax.dot_general(src[0, own_slot], image[...], (((1,), (1,)), ((), ())), preferred_element_type=jnp.float32)
    half = width // 2
    gall[me] = jnp.concatenate([gram_part_sum[:half], gram_part_sum[half:]], axis=1)

    def gram_copy(d):
        other = lax.rem(me + d, 8)
        return remote(gall.at[me], gall.at[me], gsend_sem.at[d], grecv_sem.at[me], (other // 2, lax.rem(other, 2)))

    for d in range(1, 8):
        gram_copy(d).start()
    for d in range(1, 8):
        origin = lax.rem(me + d, 8)
        remote(gall.at[origin], gall.at[origin], gsend_sem.at[d], grecv_sem.at[origin], (chip, core)).wait_recv()
    total = gall[0]
    for d in range(1, 8):
        total = total + gall[d]
    total = total / (8 * piece)
    g_out[:half] = total[:, :width]
    g_out[half:] = total[:, width:]
    for d in range(1, 8):
        gram_copy(d).wait_send()


def solution(mesh):
    def local_filter(mat_tile, y_start, center, half_width):
        piece, width = y_start.shape
        rows, cols = mat_tile.shape
        padded = -(-cols // 512) * 512
        y_t, gram = pl.pallas_call(
            functools.partial(filter_kernel, piece, width),
            out_shape=(pltpu.VMEM((width, piece), jnp.float32), pltpu.VMEM((width, width), jnp.float32)),
            in_specs=[pl.BlockSpec(memory_space=pl.ANY)] * 2 + [pl.BlockSpec(memory_space=pltpu.SMEM)] * 2,
            out_specs=(pl.BlockSpec(memory_space=pltpu.VMEM),) * 2,
            scratch_shapes=[
                pltpu.VMEM((rows, padded), jnp.bfloat16),
                pltpu.VMEM((2, 5, width, piece), jnp.bfloat16),
                pltpu.VMEM((2, width, piece), jnp.float32),
                pltpu.VMEM((width, padded), jnp.float32),
                pltpu.VMEM((2, width, piece), jnp.float32),
                pltpu.VMEM((8, width // 2, 2 * width), jnp.float32),
                pltpu.VMEM((width, piece), jnp.bfloat16),
                pltpu.SemaphoreType.DMA((2, 2, CHUNKS, 2)),
                pltpu.SemaphoreType.DMA((2, 4, CHUNKS)),
                pltpu.SemaphoreType.DMA((3, CHUNKS)),
                pltpu.SemaphoreType.DMA((2, CHUNKS)),
                pltpu.SemaphoreType.DMA((CHUNKS,)),
                pltpu.SemaphoreType.DMA((2, CHUNKS)),
                pltpu.SemaphoreType.DMA((8,)),
                pltpu.SemaphoreType.DMA((8,)),
                pltpu.SemaphoreType.DMA,
            ],
            compiler_params=pltpu.CompilerParams(collective_id=0, has_side_effects=True, vmem_limit_bytes=56 * 1024 * 1024),
            name="filter",
        )(mat_tile, y_start.T, center, half_width)
        return y_t.T, gram

    return jax.shard_map(local_filter, mesh=mesh, in_specs=(P("row", "col"), P(("col", "row"), None), P(), P()), out_specs=(P(("col", "row"), None), P()), check_vma=False)
```

```python
import functools

import jax
import jax.numpy as jnp
from jax import lax
from jax.experimental import pallas as pl
from jax.experimental.pallas import tpu as pltpu
from jax.sharding import PartitionSpec as P

DEGREE = 8
WIDTHS = (256, 256, 256, 256, 256, 128)
OFFSETS = (0, 256, 512, 768, 1024, 1280)
CHUNKS = len(WIDTHS)
MESH = pl.DeviceIdType.MESH
EARLY, LATE = 0, 1
BLOCKS = (
    (((EARLY, 0, 0),), ((EARLY, 1, 2),), ((EARLY, 3, 3), (LATE, 0, 0)), ((LATE, 1, 1), (EARLY, 4, 4)), ((EARLY, 5, 5), (LATE, 2, 3)), ((LATE, 4, 5),)),
    (((EARLY, 1, 1), (EARLY, 3, 3), (LATE, 0, 0)), ((EARLY, 5, 5), (LATE, 2, 2), (LATE, 4, 4)), ((EARLY, 0, 0), (EARLY, 2, 2), (LATE, 1, 1)), ((EARLY, 4, 4), (LATE, 3, 3)), ((LATE, 5, 5),)),
)
PASSED = (((EARLY, 0), (EARLY, 2), (LATE, 1)), ((EARLY, 4), (LATE, 3)), ((LATE, 5),), (), ())


def filter_kernel(piece, width, a_ref, y0_ref, c_ref, e_ref, y_out, g_out, tile, src, state, acc, prec, gall, image, tile_sem, recv_sem, send_sem, fwd_sem, psend_sem, prec_sem, gsend_sem, grecv_sem, y_sem):
    chip = lax.axis_index("col")
    core = lax.axis_index("row")
    me = chip * 2 + core
    sibling = 1 - core
    chip_bit = lax.rem(chip, 2)
    chip_x = chip + 1 - 2 * chip_bit
    chip_y = lax.rem(chip + 2, 4)
    group = chip // 2
    near_int = 1 - lax.abs(core - group)
    near = near_int == 1
    far = near_int == 0

    own_dest = 2 * chip_bit + core
    own_slot = near_int * own_dest + (1 - near_int) * 4
    pair_base = (2 * chip_bit, 2 * (1 - chip_bit))
    fwd_chip = near_int * chip_y + (1 - near_int) * chip_x

    def slot_of(step, kind):
        return pair_base[step] + (core if kind == LATE else sibling)

    def tile_load(step, kind, c, half):
        col = core if half else sibling
        rows = pl.ds(pl.multiple_of(slot_of(step, kind) * piece + OFFSETS[c], 128), WIDTHS[c])
        return pltpu.make_async_copy(
            a_ref.at[rows, pl.ds(pl.multiple_of(col * piece, 128), piece)],
            tile.at[rows, pl.ds(half * piece, piece)],
            tile_sem.at[step, kind, c, half],
        )

    def slot_view(par, slot, c):
        return src.at[par, slot, :, pl.ds(OFFSETS[c], WIDTHS[c])]

    def remote(src_view, dst_view, ssem, rsem, dev):
        return pltpu.make_async_remote_copy(src_ref=src_view, dst_ref=dst_view, send_sem=ssem, recv_sem=rsem, device_id=dev, device_id_type=MESH)

    def own_copy(par, c, d):
        dev = ((chip_x, group), (chip_y, group), (chip, group))[d]
        return remote(slot_view(par, own_slot, c), slot_view(par, own_dest, c), send_sem.at[d, c], recv_sem.at[par, own_dest, c], dev)

    def fwd_copy(par, step, kind, c):
        slot = slot_of(step, kind)
        return remote(slot_view(par, slot, c), slot_view(par, slot, c), fwd_sem.at[kind, c], recv_sem.at[par, slot, c], (fwd_chip, core))

    def wait_slot(par, slot, c):
        view = slot_view(par, slot, c)
        remote(view, view, fwd_sem.at[0, c], recv_sem.at[par, slot, c], (chip, core)).wait_recv()

    def partial_copy(par, o):
        cols = pl.ds(OFFSETS[o], WIDTHS[o])
        return remote(acc.at[:, cols], prec.at[par, :, cols], psend_sem.at[o], prec_sem.at[par, o], (chip, sibling))

    def send_own(par, c):
        own_copy(par, c, 0).start()
        own_copy(par, c, 1).start()

        @pl.when(far)
        def _():
            own_copy(par, c, 2).start()

    def wait_sends(par):
        for c in range(CHUNKS):
            own_copy(par, c, 0).wait_send()
            own_copy(par, c, 1).wait_send()

            @pl.when(far)
            def _():
                own_copy(par, c, 2).wait_send()

            for kind in (EARLY, LATE):

                @pl.when(near if (c + kind) % 2 == 0 else far)
                def _():
                    fwd_copy(par, 0, kind, c).wait_send()

    def arrive(par, step, kind, c):
        if step == 1:
            if (c + kind) % 2 == 0:

                @pl.when(far)
                def _():
                    wait_slot(par, slot_of(1, kind), c)

            else:
                wait_slot(par, slot_of(1, kind), c)
            return

        if kind == EARLY:
            wait_slot(par, slot_of(0, kind), c)

        if kind == LATE or (c + kind) % 2 == 1:

            @pl.when(far)
            def _():
                if kind == LATE:
                    wait_slot(par, slot_of(0, kind), c)
                if (c + kind) % 2 == 1:
                    fwd_copy(par, 0, kind, c).start()

    y0_copy = pltpu.make_async_copy(y0_ref, state.at[0], y_sem)
    y0_copy.start()

    padding = pl.ds(2 * piece, acc.shape[1] - 2 * piece)
    tile[:, padding] = jnp.zeros((tile.shape[0], padding.size), jnp.bfloat16)
    barrier = pltpu.get_barrier_semaphore()
    for d in range(1, 8):
        other = lax.rem(me + d, 8)
        pl.semaphore_signal(barrier, inc=1, device_id=(other // 2, lax.rem(other, 2)), device_id_type=MESH)

    for step in range(2):
        for kind in (EARLY, LATE):
            for c in range(CHUNKS):
                for half in range(2):
                    tile_load(step, kind, c, half).start()

    state[1] = jnp.zeros_like(state[1])
    y0_copy.wait()
    src[0, own_slot] = state[0].astype(jnp.bfloat16)
    pl.semaphore_wait(barrier, 7)
    for c in range(CHUNKS):
        send_own(0, c)
    center = c_ref[()]
    half_width = e_ref[()]

    def product(par, slot, off, size, cols):
        rows = pl.ds(pl.multiple_of(slot * piece + off, 128), size)
        return jnp.dot(src[par, slot, :, pl.ds(off, size)], tile[rows, cols], preferred_element_type=jnp.float32)

    def apply_matrix(par, first, combine):
        for step in range(2):
            for index, block in enumerate(BLOCKS[step]):
                if step == 1 and PASSED[index]:

                    @pl.when(near)
                    def _():
                        for kind, c in PASSED[index]:
                            wait_slot(par, slot_of(1, kind), c)
                            fwd_copy(par, 1, kind, c).start()

                for kind, low, high in block:
                    for c in range(low, high + 1):
                        arrive(par, step, kind, c)
                        if first:
                            for half in range(2):
                                tile_load(step, kind, c, half).wait()

                def total(cols):
                    parts = [product(par, slot_of(step, kind), OFFSETS[low], OFFSETS[high] + WIDTHS[high] - OFFSETS[low], cols) for kind, low, high in block]
                    return sum(parts[1:], parts[0])

                if step == 0 and index == 0:
                    acc[...] = total(pl.ds(0, acc.shape[1]))
                else:
                    acc[...] += total(pl.ds(0, acc.shape[1]))
        for o in range(CHUNKS):
            partial_copy(par, o).start()
        wait_sends(par)
        for o in range(CHUNKS):
            partial_copy(par, o).wait_recv()
            combine(o, acc[:, pl.ds(piece + OFFSETS[o], WIDTHS[o])] + prec[par, :, pl.ds(OFFSETS[o], WIDTHS[o])])
        for o in range(CHUNKS):
            partial_copy(par, o).wait_send()

    def advance(par, first):
        other = 1 - par

        def combine(o, total):
            cols = pl.ds(OFFSETS[o], WIDTHS[o])
            shifted = total - center * state[par, :, cols]
            if first:
                following = shifted / half_width
            else:
                following = 2.0 * shifted / half_width - state[other, :, cols]
            state[other, :, cols] = following
            src[other, own_slot, :, cols] = following.astype(jnp.bfloat16)
            send_own(other, o)

        apply_matrix(par, first, combine)

    advance(0, True)

    def step(t, carry):
        advance(lax.rem(t, 2), False)
        return carry

    lax.fori_loop(1, DEGREE, step, 0)

    y_out[...] = state[0]

    def gram_part(o, total):
        image[:, pl.ds(OFFSETS[o], WIDTHS[o])] = total.astype(jnp.bfloat16)

    apply_matrix(0, False, gram_part)
    gram_part_sum = lax.dot_general(src[0, own_slot], image[...], (((1,), (1,)), ((), ())), preferred_element_type=jnp.float32)
    half = width // 2
    gall[me] = jnp.concatenate([gram_part_sum[:half], gram_part_sum[half:]], axis=1)

    def gram_copy(d):
        other = lax.rem(me + d, 8)
        return remote(gall.at[me], gall.at[me], gsend_sem.at[d], grecv_sem.at[me], (other // 2, lax.rem(other, 2)))

    for d in range(1, 8):
        gram_copy(d).start()
    for d in range(1, 8):
        origin = lax.rem(me + d, 8)
        remote(gall.at[origin], gall.at[origin], gsend_sem.at[d], grecv_sem.at[origin], (chip, core)).wait_recv()
    total = gall[0]
    for d in range(1, 8):
        total = total + gall[d]
    total = total / (8 * piece)
    g_out[:half] = total[:, :width]
    g_out[half:] = total[:, width:]
    for d in range(1, 8):
        gram_copy(d).wait_send()


def solution(mesh):
    def local_filter(mat_tile, y_start, center, half_width):
        piece, width = y_start.shape
        rows, cols = mat_tile.shape
        padded = -(-cols // 512) * 512
        y_t, gram = pl.pallas_call(
            functools.partial(filter_kernel, piece, width),
            out_shape=(pltpu.VMEM((width, piece), jnp.float32), pltpu.VMEM((width, width), jnp.float32)),
            in_specs=[pl.BlockSpec(memory_space=pl.ANY)] * 2 + [pl.BlockSpec(memory_space=pltpu.SMEM)] * 2,
            out_specs=(pl.BlockSpec(memory_space=pltpu.VMEM),) * 2,
            scratch_shapes=[
                pltpu.VMEM((rows, padded + 128), jnp.bfloat16),
                pltpu.VMEM((2, 5, width, piece), jnp.bfloat16),
                pltpu.VMEM((2, width, piece), jnp.float32),
                pltpu.VMEM((width, padded), jnp.float32),
                pltpu.VMEM((2, width, piece), jnp.float32),
                pltpu.VMEM((8, width // 2, 2 * width), jnp.float32),
                pltpu.VMEM((width, piece), jnp.bfloat16),
                pltpu.SemaphoreType.DMA((2, 2, CHUNKS, 2)),
                pltpu.SemaphoreType.DMA((2, 4, CHUNKS)),
                pltpu.SemaphoreType.DMA((3, CHUNKS)),
                pltpu.SemaphoreType.DMA((2, CHUNKS)),
                pltpu.SemaphoreType.DMA((CHUNKS,)),
                pltpu.SemaphoreType.DMA((2, CHUNKS)),
                pltpu.SemaphoreType.DMA((8,)),
                pltpu.SemaphoreType.DMA((8,)),
                pltpu.SemaphoreType.DMA,
            ],
            compiler_params=pltpu.CompilerParams(collective_id=0, has_side_effects=True, vmem_limit_bytes=56 * 1024 * 1024),
            name="filter",
        )(mat_tile, y_start.T, center, half_width)
        return y_t.T, gram

    return jax.shard_map(local_filter, mesh=mesh, in_specs=(P("row", "col"), P(("col", "row"), None), P(), P()), out_specs=(P(("col", "row"), None), P()), check_vma=False)
```

```python
import functools

import jax
import jax.numpy as jnp
from jax import lax
from jax.experimental import pallas as pl
from jax.experimental.pallas import tpu as pltpu
from jax.sharding import PartitionSpec as P

DEGREE = 8
WIDTHS = (256, 256, 256, 256, 256, 128)
OFFSETS = (0, 256, 512, 768, 1024, 1280)
CHUNKS = len(WIDTHS)
MESH = pl.DeviceIdType.MESH
EARLY, LATE = 0, 1
BLOCKS = (
    (((EARLY, 0, 0),), ((EARLY, 1, 2),), ((LATE, 0, 0), (EARLY, 3, 3)), ((LATE, 1, 1), (EARLY, 4, 5)), ((LATE, 2, 3),), ((LATE, 4, 5),)),
    (((EARLY, 0, 1),), ((EARLY, 2, 3), (LATE, 0, 0)), ((LATE, 1, 1), (EARLY, 4, 5), (LATE, 2, 2)), ((LATE, 3, 4),), ((LATE, 5, 5),)),
)


def filter_kernel(piece, width, a_ref, y0_ref, c_ref, e_ref, y_out, g_out, tile, src, state, acc, prec, gall, image, tile_sem, recv_sem, send_sem, fwd_sem, psend_sem, prec_sem, gsend_sem, grecv_sem, y_sem):
    chip = lax.axis_index("col")
    core = lax.axis_index("row")
    me = chip * 2 + core
    sibling = 1 - core
    chip_bit = lax.rem(chip, 2)
    chip_x = chip + 1 - 2 * chip_bit
    chip_y = lax.rem(chip + 2, 4)
    group = chip // 2
    near_int = 1 - lax.abs(core - group)
    near = near_int == 1
    far = near_int == 0

    own_dest = 2 * chip_bit + core
    own_slot = near_int * own_dest + (1 - near_int) * 4
    pair_base = (2 * chip_bit, 2 * (1 - chip_bit))
    fwd_chip = near_int * chip_y + (1 - near_int) * chip_x

    def slot_of(step, kind):
        return pair_base[step] + (core if kind == LATE else sibling)

    def tile_load(step, kind, c, half):
        col = core if half else sibling
        rows = pl.ds(pl.multiple_of(slot_of(step, kind) * piece + OFFSETS[c], 128), WIDTHS[c])
        return pltpu.make_async_copy(
            a_ref.at[rows, pl.ds(pl.multiple_of(col * piece, 128), piece)],
            tile.at[rows, pl.ds(half * piece, piece)],
            tile_sem.at[step, kind, c, half],
        )

    def slot_view(par, slot, c):
        return src.at[par, slot, :, pl.ds(OFFSETS[c], WIDTHS[c])]

    def remote(src_view, dst_view, ssem, rsem, dev):
        return pltpu.make_async_remote_copy(src_ref=src_view, dst_ref=dst_view, send_sem=ssem, recv_sem=rsem, device_id=dev, device_id_type=MESH)

    def own_copy(par, c, d):
        dev = ((chip_x, group), (chip_y, group), (chip, group))[d]
        return remote(slot_view(par, own_slot, c), slot_view(par, own_dest, c), send_sem.at[d, c], recv_sem.at[par, own_dest, c], dev)

    def fwd_copy(par, step, kind, c):
        slot = slot_of(step, kind)
        return remote(slot_view(par, slot, c), slot_view(par, slot, c), fwd_sem.at[kind, c], recv_sem.at[par, slot, c], (fwd_chip, core))

    def wait_slot(par, slot, c):
        view = slot_view(par, slot, c)
        remote(view, view, fwd_sem.at[0, c], recv_sem.at[par, slot, c], (chip, core)).wait_recv()

    def partial_copy(par, o):
        cols = pl.ds(OFFSETS[o], WIDTHS[o])
        return remote(acc.at[:, cols], prec.at[par, :, cols], psend_sem.at[o], prec_sem.at[par, o], (chip, sibling))

    def send_own(par, c):
        own_copy(par, c, 0).start()
        own_copy(par, c, 1).start()

        @pl.when(far)
        def _():
            own_copy(par, c, 2).start()

    def wait_sends(par):
        for c in range(CHUNKS):
            own_copy(par, c, 0).wait_send()
            own_copy(par, c, 1).wait_send()

            @pl.when(far)
            def _():
                own_copy(par, c, 2).wait_send()

            for kind in (EARLY, LATE):

                @pl.when(near if (c + kind) % 2 == 0 else far)
                def _():
                    fwd_copy(par, 0, kind, c).wait_send()

    def arrive(par, step, kind, c):
        if step == 1:
            wait_slot(par, slot_of(1, kind), c)
            if (c + kind) % 2 == 0:

                @pl.when(near)
                def _():
                    fwd_copy(par, 1, kind, c).start()

            return

        if kind == EARLY:
            wait_slot(par, slot_of(0, kind), c)

        if kind == LATE or (c + kind) % 2 == 1:

            @pl.when(far)
            def _():
                if kind == LATE:
                    wait_slot(par, slot_of(0, kind), c)
                if (c + kind) % 2 == 1:
                    fwd_copy(par, 0, kind, c).start()

    y0_copy = pltpu.make_async_copy(y0_ref, state.at[0], y_sem)
    y0_copy.start()

    padding = pl.ds(2 * piece, acc.shape[1] - 2 * piece)
    tile[:, padding] = jnp.zeros((tile.shape[0], padding.size), jnp.bfloat16)
    barrier = pltpu.get_barrier_semaphore()
    for d in range(1, 8):
        other = lax.rem(me + d, 8)
        pl.semaphore_signal(barrier, inc=1, device_id=(other // 2, lax.rem(other, 2)), device_id_type=MESH)

    for step in range(2):
        for kind in (EARLY, LATE):
            for c in range(CHUNKS):
                for half in range(2):
                    tile_load(step, kind, c, half).start()

    state[1] = jnp.zeros_like(state[1])
    y0_copy.wait()
    src[0, own_slot] = state[0].astype(jnp.bfloat16)
    pl.semaphore_wait(barrier, 7)
    for c in range(CHUNKS):
        send_own(0, c)
    center = c_ref[()]
    half_width = e_ref[()]

    def product(par, slot, off, size, cols):
        rows = pl.ds(pl.multiple_of(slot * piece + off, 128), size)
        return jnp.dot(src[par, slot, :, pl.ds(off, size)], tile[rows, cols], preferred_element_type=jnp.float32)

    def apply_matrix(par, first, combine):
        for step in range(2):
            for index, block in enumerate(BLOCKS[step]):
                for kind, low, high in block:
                    for c in range(low, high + 1):
                        arrive(par, step, kind, c)
                        if first:
                            for half in range(2):
                                tile_load(step, kind, c, half).wait()

                def total(cols):
                    parts = [product(par, slot_of(step, kind), OFFSETS[low], OFFSETS[high] + WIDTHS[high] - OFFSETS[low], cols) for kind, low, high in block]
                    return sum(parts[1:], parts[0])

                if step == 0 and index == 0:
                    acc[...] = total(pl.ds(0, acc.shape[1]))
                else:
                    acc[...] += total(pl.ds(0, acc.shape[1]))
        for o in range(CHUNKS):
            partial_copy(par, o).start()
        wait_sends(par)
        for o in range(CHUNKS):
            partial_copy(par, o).wait_recv()
            combine(o, acc[:, pl.ds(piece + OFFSETS[o], WIDTHS[o])] + prec[par, :, pl.ds(OFFSETS[o], WIDTHS[o])])
        for o in range(CHUNKS):
            partial_copy(par, o).wait_send()

    def advance(par, first):
        other = 1 - par

        def combine(o, total):
            cols = pl.ds(OFFSETS[o], WIDTHS[o])
            shifted = total - center * state[par, :, cols]
            if first:
                following = shifted / half_width
            else:
                following = 2.0 * shifted / half_width - state[other, :, cols]
            state[other, :, cols] = following
            src[other, own_slot, :, cols] = following.astype(jnp.bfloat16)
            send_own(other, o)

        apply_matrix(par, first, combine)

    advance(0, True)

    def step(t, carry):
        advance(lax.rem(t, 2), False)
        return carry

    lax.fori_loop(1, DEGREE, step, 0)

    y_out[...] = state[0]

    def gram_part(o, total):
        image[:, pl.ds(OFFSETS[o], WIDTHS[o])] = total.astype(jnp.bfloat16)

    apply_matrix(0, False, gram_part)
    gram_part_sum = lax.dot_general(src[0, own_slot], image[...], (((1,), (1,)), ((), ())), preferred_element_type=jnp.float32)
    half = width // 2
    gall[me] = jnp.concatenate([gram_part_sum[:half], gram_part_sum[half:]], axis=1)

    def gram_copy(d):
        other = lax.rem(me + d, 8)
        return remote(gall.at[me], gall.at[me], gsend_sem.at[d], grecv_sem.at[me], (other // 2, lax.rem(other, 2)))

    for d in range(1, 8):
        gram_copy(d).start()
    for d in range(1, 8):
        origin = lax.rem(me + d, 8)
        remote(gall.at[origin], gall.at[origin], gsend_sem.at[d], grecv_sem.at[origin], (chip, core)).wait_recv()
    total = gall[0]
    for d in range(1, 8):
        total = total + gall[d]
    total = total / (8 * piece)
    g_out[:half] = total[:, :width]
    g_out[half:] = total[:, width:]
    for d in range(1, 8):
        gram_copy(d).wait_send()


def solution(mesh):
    def local_filter(mat_tile, y_start, center, half_width):
        piece, width = y_start.shape
        rows, cols = mat_tile.shape
        padded = -(-cols // 512) * 512
        y_t, gram = pl.pallas_call(
            functools.partial(filter_kernel, piece, width),
            out_shape=(pltpu.VMEM((width, piece), jnp.float32), pltpu.VMEM((width, width), jnp.float32)),
            in_specs=[pl.BlockSpec(memory_space=pl.ANY)] * 2 + [pl.BlockSpec(memory_space=pltpu.SMEM)] * 2,
            out_specs=(pl.BlockSpec(memory_space=pltpu.VMEM),) * 2,
            scratch_shapes=[
                pltpu.VMEM((rows, padded + 128), jnp.bfloat16),
                pltpu.VMEM((2, 5, width, piece), jnp.bfloat16),
                pltpu.VMEM((2, width, piece), jnp.float32),
                pltpu.VMEM((width, padded), jnp.float32),
                pltpu.VMEM((2, width, piece), jnp.float32),
                pltpu.VMEM((8, width // 2, 2 * width), jnp.float32),
                pltpu.VMEM((width, piece), jnp.bfloat16),
                pltpu.SemaphoreType.DMA((2, 2, CHUNKS, 2)),
                pltpu.SemaphoreType.DMA((2, 4, CHUNKS)),
                pltpu.SemaphoreType.DMA((3, CHUNKS)),
                pltpu.SemaphoreType.DMA((2, CHUNKS)),
                pltpu.SemaphoreType.DMA((CHUNKS,)),
                pltpu.SemaphoreType.DMA((2, CHUNKS)),
                pltpu.SemaphoreType.DMA((8,)),
                pltpu.SemaphoreType.DMA((8,)),
                pltpu.SemaphoreType.DMA,
            ],
            compiler_params=pltpu.CompilerParams(collective_id=0, has_side_effects=True, vmem_limit_bytes=56 * 1024 * 1024),
            name="filter",
        )(mat_tile, y_start.T, center, half_width)
        return y_t.T, gram

    return jax.shard_map(local_filter, mesh=mesh, in_specs=(P("row", "col"), P(("col", "row"), None), P(), P()), out_specs=(P(("col", "row"), None), P()), check_vma=False)
```

```python
import functools

import jax
import jax.numpy as jnp
from jax import lax
from jax.experimental import pallas as pl
from jax.experimental.pallas import tpu as pltpu
from jax.sharding import PartitionSpec as P

DEGREE = 8
WIDTHS = (256, 256, 256, 256, 256, 128)
OFFSETS = (0, 256, 512, 768, 1024, 1280)
CHUNKS = len(WIDTHS)
MESH = pl.DeviceIdType.MESH
EARLY, LATE = 0, 1
BLOCKS = (
    (((EARLY, 0, 0),), ((EARLY, 1, 2),), ((LATE, 0, 0), (EARLY, 3, 3)), ((LATE, 1, 2),), ((EARLY, 4, 5), (LATE, 3, 3)), ((LATE, 4, 5),)),
    (((EARLY, 0, 1),), ((EARLY, 2, 3), (LATE, 0, 0)), ((LATE, 1, 1), (EARLY, 4, 5), (LATE, 2, 2)), ((LATE, 3, 5),)),
)


def filter_kernel(piece, width, a_ref, y0_ref, c_ref, e_ref, y_out, g_out, tile, src, state, acc, prec, gall, image, tile_sem, recv_sem, send_sem, fwd_sem, psend_sem, prec_sem, gsend_sem, grecv_sem, y_sem):
    chip = lax.axis_index("col")
    core = lax.axis_index("row")
    me = chip * 2 + core
    sibling = 1 - core
    chip_bit = lax.rem(chip, 2)
    chip_x = chip + 1 - 2 * chip_bit
    chip_y = lax.rem(chip + 2, 4)
    group = chip // 2
    near_int = 1 - lax.abs(core - group)
    near = near_int == 1
    far = near_int == 0

    own_dest = 2 * chip_bit + core
    own_slot = near_int * own_dest + (1 - near_int) * 4
    pair_base = (2 * chip_bit, 2 * (1 - chip_bit))
    fwd_chip = near_int * chip_y + (1 - near_int) * chip_x

    def slot_of(step, kind):
        return pair_base[step] + (core if kind == LATE else sibling)

    def tile_load(step, kind, half):
        col = core if half else sibling
        rows = pl.ds(pl.multiple_of(slot_of(step, kind) * piece, 128), piece)
        return pltpu.make_async_copy(
            a_ref.at[rows, pl.ds(pl.multiple_of(col * piece, 128), piece)],
            tile.at[rows, pl.ds(half * piece, piece)],
            tile_sem.at[step, kind, half],
        )

    def slot_view(par, slot, c):
        return src.at[par, slot, :, pl.ds(OFFSETS[c], WIDTHS[c])]

    def remote(src_view, dst_view, ssem, rsem, dev):
        return pltpu.make_async_remote_copy(src_ref=src_view, dst_ref=dst_view, send_sem=ssem, recv_sem=rsem, device_id=dev, device_id_type=MESH)

    def own_copy(par, c, d):
        dev = ((chip_x, group), (chip_y, group), (chip, group))[d]
        return remote(slot_view(par, own_slot, c), slot_view(par, own_dest, c), send_sem.at[d, c], recv_sem.at[par, own_dest, c], dev)

    def fwd_copy(par, step, kind, c):
        slot = slot_of(step, kind)
        return remote(slot_view(par, slot, c), slot_view(par, slot, c), fwd_sem.at[kind, c], recv_sem.at[par, slot, c], (fwd_chip, core))

    def wait_slot(par, slot, c):
        view = slot_view(par, slot, c)
        remote(view, view, fwd_sem.at[0, c], recv_sem.at[par, slot, c], (chip, core)).wait_recv()

    def partial_copy(par, o):
        cols = pl.ds(OFFSETS[o], WIDTHS[o])
        return remote(acc.at[:, cols], prec.at[par, :, cols], psend_sem.at[o], prec_sem.at[par, o], (chip, sibling))

    def send_own(par, c):
        own_copy(par, c, 0).start()
        own_copy(par, c, 1).start()

        @pl.when(far)
        def _():
            own_copy(par, c, 2).start()

    def wait_sends(par):
        for c in range(CHUNKS):
            own_copy(par, c, 0).wait_send()
            own_copy(par, c, 1).wait_send()

            @pl.when(far)
            def _():
                own_copy(par, c, 2).wait_send()

            for kind in (EARLY, LATE):

                @pl.when(near if (c + kind) % 2 == 0 else far)
                def _():
                    fwd_copy(par, 0, kind, c).wait_send()

    def arrive(par, step, kind, c):
        if step == 1:
            wait_slot(par, slot_of(1, kind), c)
            if (c + kind) % 2 == 0:

                @pl.when(near)
                def _():
                    fwd_copy(par, 1, kind, c).start()

            return

        if kind == EARLY:
            wait_slot(par, slot_of(0, kind), c)

        if kind == LATE or (c + kind) % 2 == 1:

            @pl.when(far)
            def _():
                if kind == LATE:
                    wait_slot(par, slot_of(0, kind), c)
                if (c + kind) % 2 == 1:
                    fwd_copy(par, 0, kind, c).start()

    y0_copy = pltpu.make_async_copy(y0_ref, state.at[0], y_sem)
    y0_copy.start()

    barrier = pltpu.get_barrier_semaphore()
    for d in range(1, 8):
        other = lax.rem(me + d, 8)
        pl.semaphore_signal(barrier, inc=1, device_id=(other // 2, lax.rem(other, 2)), device_id_type=MESH)

    for step in range(2):
        for kind in (EARLY, LATE):
            for half in range(2):
                tile_load(step, kind, half).start()

    state[1] = jnp.zeros_like(state[1])
    y0_copy.wait()
    src[0, own_slot] = state[0].astype(jnp.bfloat16)
    pl.semaphore_wait(barrier, 7)
    for c in range(CHUNKS):
        send_own(0, c)
    center = c_ref[()]
    half_width = e_ref[()]

    def product(par, slot, off, size, cols):
        rows = pl.ds(pl.multiple_of(slot * piece + off, 128), size)
        return jnp.dot(src[par, slot, :, pl.ds(off, size)], tile[rows, cols], preferred_element_type=jnp.float32)

    def apply_matrix(par, first, combine):
        for step in range(2):
            for index, block in enumerate(BLOCKS[step]):
                for kind, low, high in block:
                    for c in range(low, high + 1):
                        arrive(par, step, kind, c)
                        if first and c == 0:
                            for half in range(2):
                                tile_load(step, kind, half).wait()

                def total(cols):
                    parts = [product(par, slot_of(step, kind), OFFSETS[low], OFFSETS[high] + WIDTHS[high] - OFFSETS[low], cols) for kind, low, high in block]
                    return sum(parts[1:], parts[0])

                if step == 0 and index == 0:
                    acc[...] = total(slice(None))
                else:
                    acc[...] += total(slice(None))
        for o in range(CHUNKS):
            partial_copy(par, o).start()
        wait_sends(par)
        for o in range(CHUNKS):
            partial_copy(par, o).wait_recv()
            combine(o, acc[:, pl.ds(piece + OFFSETS[o], WIDTHS[o])] + prec[par, :, pl.ds(OFFSETS[o], WIDTHS[o])])
        for o in range(CHUNKS):
            partial_copy(par, o).wait_send()

    def advance(par, first):
        other = 1 - par

        def combine(o, total):
            cols = pl.ds(OFFSETS[o], WIDTHS[o])
            shifted = total - center * state[par, :, cols]
            if first:
                following = shifted / half_width
            else:
                following = 2.0 * shifted / half_width - state[other, :, cols]
            state[other, :, cols] = following
            src[other, own_slot, :, cols] = following.astype(jnp.bfloat16)
            send_own(other, o)

        apply_matrix(par, first, combine)

    advance(0, True)

    def step(t, carry):
        advance(lax.rem(t, 2), False)
        return carry

    lax.fori_loop(1, DEGREE, step, 0)

    y_out[...] = state[0]

    def gram_part(o, total):
        image[:, pl.ds(OFFSETS[o], WIDTHS[o])] = total.astype(jnp.bfloat16)

    apply_matrix(0, False, gram_part)
    gram_part_sum = lax.dot_general(src[0, own_slot], image[...], (((1,), (1,)), ((), ())), preferred_element_type=jnp.float32)
    half = width // 2
    gall[me] = jnp.concatenate([gram_part_sum[:half], gram_part_sum[half:]], axis=1)

    def gram_copy(d):
        other = lax.rem(me + d, 8)
        return remote(gall.at[me], gall.at[me], gsend_sem.at[d], grecv_sem.at[me], (other // 2, lax.rem(other, 2)))

    for d in range(1, 8):
        gram_copy(d).start()
    for d in range(1, 8):
        origin = lax.rem(me + d, 8)
        remote(gall.at[origin], gall.at[origin], gsend_sem.at[d], grecv_sem.at[origin], (chip, core)).wait_recv()
    total = gall[0]
    for d in range(1, 8):
        total = total + gall[d]
    total = total / (8 * piece)
    g_out[:half] = total[:, :width]
    g_out[half:] = total[:, width:]
    for d in range(1, 8):
        gram_copy(d).wait_send()


def solution(mesh):
    def local_filter(mat_tile, y_start, center, half_width):
        piece, width = y_start.shape
        rows, cols = mat_tile.shape
        y_t, gram = pl.pallas_call(
            functools.partial(filter_kernel, piece, width),
            out_shape=(pltpu.VMEM((width, piece), jnp.float32), pltpu.VMEM((width, width), jnp.float32)),
            in_specs=[pl.BlockSpec(memory_space=pl.ANY)] * 2 + [pl.BlockSpec(memory_space=pltpu.SMEM)] * 2,
            out_specs=(pl.BlockSpec(memory_space=pltpu.VMEM),) * 2,
            scratch_shapes=[
                pltpu.VMEM((rows, cols), jnp.bfloat16),
                pltpu.VMEM((2, 5, width, piece), jnp.bfloat16),
                pltpu.VMEM((2, width, piece), jnp.float32),
                pltpu.VMEM((width, cols), jnp.float32),
                pltpu.VMEM((2, width, piece), jnp.float32),
                pltpu.VMEM((8, width // 2, 2 * width), jnp.float32),
                pltpu.VMEM((width, piece), jnp.bfloat16),
                pltpu.SemaphoreType.DMA((2, 2, 2)),
                pltpu.SemaphoreType.DMA((2, 4, CHUNKS)),
                pltpu.SemaphoreType.DMA((3, CHUNKS)),
                pltpu.SemaphoreType.DMA((2, CHUNKS)),
                pltpu.SemaphoreType.DMA((CHUNKS,)),
                pltpu.SemaphoreType.DMA((2, CHUNKS)),
                pltpu.SemaphoreType.DMA((8,)),
                pltpu.SemaphoreType.DMA((8,)),
                pltpu.SemaphoreType.DMA,
            ],
            compiler_params=pltpu.CompilerParams(collective_id=0, has_side_effects=True, vmem_limit_bytes=56 * 1024 * 1024),
            name="filter",
        )(mat_tile, y_start.T, center, half_width)
        return y_t.T, gram

    return jax.shard_map(local_filter, mesh=mesh, in_specs=(P("row", "col"), P(("col", "row"), None), P(), P()), out_specs=(P(("col", "row"), None), P()), check_vma=False)
```

```python
import functools

import jax
import jax.numpy as jnp
from jax import lax
from jax.experimental import pallas as pl
from jax.experimental.pallas import tpu as pltpu
from jax.sharding import PartitionSpec as P

DEGREE = 8
WIDTHS = (256, 256, 256, 256, 256, 128)
OFFSETS = (0, 256, 512, 768, 1024, 1280)
CHUNKS = len(WIDTHS)
MESH = pl.DeviceIdType.MESH
EARLY, LATE = 0, 1
BLOCKS = (
    (((EARLY, 0, 0),), ((EARLY, 1, 2),), ((LATE, 0, 0), (EARLY, 3, 3)), ((LATE, 1, 1), (EARLY, 4, 5)), ((LATE, 2, 3),), ((LATE, 4, 5),)),
    (((EARLY, 0, 1),), ((EARLY, 2, 3), (LATE, 0, 0)), ((LATE, 1, 1), (EARLY, 4, 5), (LATE, 2, 2)), ((LATE, 3, 5),)),
)


def filter_kernel(piece, width, a_ref, y0_ref, c_ref, e_ref, y_out, g_out, tile, src, state, acc, prec, gall, image, tile_sem, recv_sem, send_sem, fwd_sem, psend_sem, prec_sem, gsend_sem, grecv_sem, y_sem):
    chip = lax.axis_index("col")
    core = lax.axis_index("row")
    me = chip * 2 + core
    sibling = 1 - core
    chip_bit = lax.rem(chip, 2)
    chip_x = chip + 1 - 2 * chip_bit
    chip_y = lax.rem(chip + 2, 4)
    group = chip // 2
    near_int = 1 - lax.abs(core - group)
    near = near_int == 1
    far = near_int == 0

    own_dest = 2 * chip_bit + core
    own_slot = near_int * own_dest + (1 - near_int) * 4
    pair_base = (2 * chip_bit, 2 * (1 - chip_bit))
    fwd_chip = near_int * chip_y + (1 - near_int) * chip_x

    def slot_of(step, kind):
        return pair_base[step] + (core if kind == LATE else sibling)

    def tile_load(step, kind, c, half):
        col = core if half else sibling
        rows = pl.ds(pl.multiple_of(slot_of(step, kind) * piece + OFFSETS[c], 128), WIDTHS[c])
        return pltpu.make_async_copy(
            a_ref.at[rows, pl.ds(pl.multiple_of(col * piece, 128), piece)],
            tile.at[rows, pl.ds(half * piece, piece)],
            tile_sem.at[step, kind, c, half],
        )

    def slot_view(par, slot, c):
        return src.at[par, slot, :, pl.ds(OFFSETS[c], WIDTHS[c])]

    def remote(src_view, dst_view, ssem, rsem, dev):
        return pltpu.make_async_remote_copy(src_ref=src_view, dst_ref=dst_view, send_sem=ssem, recv_sem=rsem, device_id=dev, device_id_type=MESH)

    def own_copy(par, c, d):
        dev = ((chip_x, group), (chip_y, group), (chip, group))[d]
        return remote(slot_view(par, own_slot, c), slot_view(par, own_dest, c), send_sem.at[d, c], recv_sem.at[par, own_dest, c], dev)

    def fwd_copy(par, step, kind, c):
        slot = slot_of(step, kind)
        return remote(slot_view(par, slot, c), slot_view(par, slot, c), fwd_sem.at[kind, c], recv_sem.at[par, slot, c], (fwd_chip, core))

    def wait_slot(par, slot, c):
        view = slot_view(par, slot, c)
        remote(view, view, fwd_sem.at[0, c], recv_sem.at[par, slot, c], (chip, core)).wait_recv()

    def partial_copy(par, o):
        cols = pl.ds(OFFSETS[o], WIDTHS[o])
        return remote(acc.at[:, cols], prec.at[par, :, cols], psend_sem.at[o], prec_sem.at[par, o], (chip, sibling))

    def send_own(par, c):
        own_copy(par, c, 0).start()
        own_copy(par, c, 1).start()

        @pl.when(far)
        def _():
            own_copy(par, c, 2).start()

    def wait_sends(par):
        for c in range(CHUNKS):
            own_copy(par, c, 0).wait_send()
            own_copy(par, c, 1).wait_send()

            @pl.when(far)
            def _():
                own_copy(par, c, 2).wait_send()

            for kind in (EARLY, LATE):

                @pl.when(near if (c + kind) % 2 == 0 else far)
                def _():
                    fwd_copy(par, 0, kind, c).wait_send()

    def arrive(par, step, kind, c):
        if step == 1:
            if kind == EARLY and c % 2 == 0:

                @pl.when(far)
                def _():
                    wait_slot(par, slot_of(1, kind), c)

                return

            wait_slot(par, slot_of(1, kind), c)
            if (c + kind) % 2 == 0:

                @pl.when(near)
                def _():
                    fwd_copy(par, 1, kind, c).start()

            return

        if kind == EARLY:
            wait_slot(par, slot_of(0, kind), c)

        if kind == LATE or (c + kind) % 2 == 1:

            @pl.when(far)
            def _():
                if kind == LATE:
                    wait_slot(par, slot_of(0, kind), c)
                if (c + kind) % 2 == 1:
                    fwd_copy(par, 0, kind, c).start()

    y0_copy = pltpu.make_async_copy(y0_ref, state.at[0], y_sem)
    y0_copy.start()

    barrier = pltpu.get_barrier_semaphore()
    for d in range(1, 8):
        other = lax.rem(me + d, 8)
        pl.semaphore_signal(barrier, inc=1, device_id=(other // 2, lax.rem(other, 2)), device_id_type=MESH)

    for step in range(2):
        for kind in (EARLY, LATE):
            for c in range(CHUNKS):
                for half in range(2):
                    tile_load(step, kind, c, half).start()

    state[1] = jnp.zeros_like(state[1])
    y0_copy.wait()
    src[0, own_slot] = state[0].astype(jnp.bfloat16)
    pl.semaphore_wait(barrier, 7)
    for c in range(CHUNKS):
        send_own(0, c)
    center = c_ref[()]
    half_width = e_ref[()]

    def product(par, slot, off, size, cols):
        rows = pl.ds(pl.multiple_of(slot * piece + off, 128), size)
        return jnp.dot(src[par, slot, :, pl.ds(off, size)], tile[rows, cols], preferred_element_type=jnp.float32)

    def apply_matrix(par, first, combine):
        for step in range(2):
            for index, block in enumerate(BLOCKS[step]):
                if step == 0 and index >= 3:

                    @pl.when(near)
                    def _():
                        wait_slot(par, slot_of(1, EARLY), 2 * index - 6)
                        fwd_copy(par, 1, EARLY, 2 * index - 6).start()

                for kind, low, high in block:
                    for c in range(low, high + 1):
                        arrive(par, step, kind, c)
                        if first:
                            for half in range(2):
                                tile_load(step, kind, c, half).wait()

                def total(cols):
                    parts = [product(par, slot_of(step, kind), OFFSETS[low], OFFSETS[high] + WIDTHS[high] - OFFSETS[low], cols) for kind, low, high in block]
                    return sum(parts[1:], parts[0])

                if step == 0 and index == 0:
                    acc[...] = total(slice(None))
                else:
                    acc[...] += total(slice(None))
        for o in range(CHUNKS):
            partial_copy(par, o).start()
        wait_sends(par)
        for o in range(CHUNKS):
            partial_copy(par, o).wait_recv()
            combine(o, acc[:, pl.ds(piece + OFFSETS[o], WIDTHS[o])] + prec[par, :, pl.ds(OFFSETS[o], WIDTHS[o])])
        for o in range(CHUNKS):
            partial_copy(par, o).wait_send()

    def advance(par, first):
        other = 1 - par

        def combine(o, total):
            cols = pl.ds(OFFSETS[o], WIDTHS[o])
            shifted = total - center * state[par, :, cols]
            if first:
                following = shifted / half_width
            else:
                following = 2.0 * shifted / half_width - state[other, :, cols]
            state[other, :, cols] = following
            src[other, own_slot, :, cols] = following.astype(jnp.bfloat16)
            send_own(other, o)

        apply_matrix(par, first, combine)

    advance(0, True)

    def step(t, carry):
        advance(lax.rem(t, 2), False)
        return carry

    lax.fori_loop(1, DEGREE, step, 0)

    y_out[...] = state[0]

    def gram_part(o, total):
        image[:, pl.ds(OFFSETS[o], WIDTHS[o])] = total.astype(jnp.bfloat16)

    apply_matrix(0, False, gram_part)
    gram_part_sum = lax.dot_general(src[0, own_slot], image[...], (((1,), (1,)), ((), ())), preferred_element_type=jnp.float32)
    half = width // 2
    gall[me] = jnp.concatenate([gram_part_sum[:half], gram_part_sum[half:]], axis=1)

    def gram_copy(d):
        other = lax.rem(me + d, 8)
        return remote(gall.at[me], gall.at[me], gsend_sem.at[d], grecv_sem.at[me], (other // 2, lax.rem(other, 2)))

    for d in range(1, 8):
        gram_copy(d).start()
    for d in range(1, 8):
        origin = lax.rem(me + d, 8)
        remote(gall.at[origin], gall.at[origin], gsend_sem.at[d], grecv_sem.at[origin], (chip, core)).wait_recv()
    total = gall[0]
    for d in range(1, 8):
        total = total + gall[d]
    total = total / (8 * piece)
    g_out[:half] = total[:, :width]
    g_out[half:] = total[:, width:]
    for d in range(1, 8):
        gram_copy(d).wait_send()


def solution(mesh):
    def local_filter(mat_tile, y_start, center, half_width):
        piece, width = y_start.shape
        rows, cols = mat_tile.shape
        y_t, gram = pl.pallas_call(
            functools.partial(filter_kernel, piece, width),
            out_shape=(pltpu.VMEM((width, piece), jnp.float32), pltpu.VMEM((width, width), jnp.float32)),
            in_specs=[pl.BlockSpec(memory_space=pl.ANY)] * 2 + [pl.BlockSpec(memory_space=pltpu.SMEM)] * 2,
            out_specs=(pl.BlockSpec(memory_space=pltpu.VMEM),) * 2,
            scratch_shapes=[
                pltpu.VMEM((rows, cols), jnp.bfloat16),
                pltpu.VMEM((2, 5, width, piece), jnp.bfloat16),
                pltpu.VMEM((2, width, piece), jnp.float32),
                pltpu.VMEM((width, cols), jnp.float32),
                pltpu.VMEM((2, width, piece), jnp.float32),
                pltpu.VMEM((8, width // 2, 2 * width), jnp.float32),
                pltpu.VMEM((width, piece), jnp.bfloat16),
                pltpu.SemaphoreType.DMA((2, 2, CHUNKS, 2)),
                pltpu.SemaphoreType.DMA((2, 4, CHUNKS)),
                pltpu.SemaphoreType.DMA((3, CHUNKS)),
                pltpu.SemaphoreType.DMA((2, CHUNKS)),
                pltpu.SemaphoreType.DMA((CHUNKS,)),
                pltpu.SemaphoreType.DMA((2, CHUNKS)),
                pltpu.SemaphoreType.DMA((8,)),
                pltpu.SemaphoreType.DMA((8,)),
                pltpu.SemaphoreType.DMA,
            ],
            compiler_params=pltpu.CompilerParams(collective_id=0, has_side_effects=True, vmem_limit_bytes=56 * 1024 * 1024),
            name="filter",
        )(mat_tile, y_start.T, center, half_width)
        return y_t.T, gram

    return jax.shard_map(local_filter, mesh=mesh, in_specs=(P("row", "col"), P(("col", "row"), None), P(), P()), out_specs=(P(("col", "row"), None), P()), check_vma=False)
```

```python
import functools

import jax
import jax.numpy as jnp
from jax import lax
from jax.experimental import pallas as pl
from jax.experimental.pallas import tpu as pltpu
from jax.sharding import PartitionSpec as P

DEGREE = 8
WIDTHS = (256, 256, 256, 256, 256, 128)
OFFSETS = (0, 256, 512, 768, 1024, 1280)
CHUNKS = len(WIDTHS)
MESH = pl.DeviceIdType.MESH
EARLY, LATE = 0, 1
BLOCKS = (
    (((EARLY, 0, 0),), ((EARLY, 1, 2),), ((LATE, 0, 0), (EARLY, 3, 3)), ((LATE, 1, 1), (EARLY, 4, 5)), ((LATE, 2, 3),), ((LATE, 4, 5),)),
    (((EARLY, 0, 1),), ((EARLY, 2, 3), (LATE, 0, 0)), ((LATE, 1, 1), (EARLY, 4, 5), (LATE, 2, 2)), ((LATE, 3, 5),)),
)
HELD_BACK = ((EARLY, 1), (EARLY, 3), (LATE, 0))
PASSED_AT_ONCE = ((EARLY, 5), (LATE, 2), (LATE, 4))


def filter_kernel(piece, width, a_ref, y0_ref, c_ref, e_ref, y_out, g_out, tile, src, state, acc, prec, gall, image, tile_sem, recv_sem, send_sem, fwd_sem, psend_sem, prec_sem, gsend_sem, grecv_sem, y_sem):
    chip = lax.axis_index("col")
    core = lax.axis_index("row")
    me = chip * 2 + core
    sibling = 1 - core
    chip_bit = lax.rem(chip, 2)
    chip_x = chip + 1 - 2 * chip_bit
    chip_y = lax.rem(chip + 2, 4)
    group = chip // 2
    near_int = 1 - lax.abs(core - group)
    near = near_int == 1
    far = near_int == 0

    own_dest = 2 * chip_bit + core
    own_slot = near_int * own_dest + (1 - near_int) * 4
    pair_base = (2 * chip_bit, 2 * (1 - chip_bit))
    fwd_chip = near_int * chip_y + (1 - near_int) * chip_x

    def slot_of(step, kind):
        return pair_base[step] + (core if kind == LATE else sibling)

    def tile_load(step, kind, c, half):
        col = core if half else sibling
        rows = pl.ds(pl.multiple_of(slot_of(step, kind) * piece + OFFSETS[c], 128), WIDTHS[c])
        return pltpu.make_async_copy(
            a_ref.at[rows, pl.ds(pl.multiple_of(col * piece, 128), piece)],
            tile.at[rows, pl.ds(half * piece, piece)],
            tile_sem.at[step, kind, c, half],
        )

    def slot_view(par, slot, c):
        return src.at[par, slot, :, pl.ds(OFFSETS[c], WIDTHS[c])]

    def remote(src_view, dst_view, ssem, rsem, dev):
        return pltpu.make_async_remote_copy(src_ref=src_view, dst_ref=dst_view, send_sem=ssem, recv_sem=rsem, device_id=dev, device_id_type=MESH)

    def own_copy(par, c, d):
        dev = ((chip_x, group), (chip_y, group), (chip, group))[d]
        return remote(slot_view(par, own_slot, c), slot_view(par, own_dest, c), send_sem.at[d, c], recv_sem.at[par, own_dest, c], dev)

    def fwd_copy(par, step, kind, c):
        slot = slot_of(step, kind)
        return remote(slot_view(par, slot, c), slot_view(par, slot, c), fwd_sem.at[kind, c], recv_sem.at[par, slot, c], (fwd_chip, core))

    def wait_slot(par, slot, c):
        view = slot_view(par, slot, c)
        remote(view, view, fwd_sem.at[0, c], recv_sem.at[par, slot, c], (chip, core)).wait_recv()

    def partial_copy(par, o):
        cols = pl.ds(OFFSETS[o], WIDTHS[o])
        return remote(acc.at[:, cols], prec.at[par, :, cols], psend_sem.at[o], prec_sem.at[par, o], (chip, sibling))

    def send_own(par, c):
        own_copy(par, c, 0).start()
        own_copy(par, c, 1).start()

        @pl.when(far)
        def _():
            own_copy(par, c, 2).start()

    def wait_sends(par):
        for c in range(CHUNKS):
            own_copy(par, c, 0).wait_send()
            own_copy(par, c, 1).wait_send()

            @pl.when(far)
            def _():
                own_copy(par, c, 2).wait_send()

            for kind in (EARLY, LATE):

                @pl.when(near if (c + kind) % 2 == 0 else far)
                def _():
                    fwd_copy(par, 0, kind, c).wait_send()

    def arrive(par, step, kind, c):
        if step == 1:
            wait_slot(par, slot_of(1, kind), c)
            if (c + kind) % 2 == 0:

                @pl.when(near)
                def _():
                    fwd_copy(par, 1, kind, c).start()

            return

        if kind == EARLY:
            wait_slot(par, slot_of(0, kind), c)

        if kind == LATE or (kind, c) in PASSED_AT_ONCE:

            @pl.when(far)
            def _():
                if kind == LATE:
                    wait_slot(par, slot_of(0, kind), c)
                if (kind, c) in PASSED_AT_ONCE:
                    fwd_copy(par, 0, kind, c).start()

    y0_copy = pltpu.make_async_copy(y0_ref, state.at[0], y_sem)
    y0_copy.start()

    barrier = pltpu.get_barrier_semaphore()
    for d in range(1, 8):
        other = lax.rem(me + d, 8)
        pl.semaphore_signal(barrier, inc=1, device_id=(other // 2, lax.rem(other, 2)), device_id_type=MESH)

    for step in range(2):
        for kind in (EARLY, LATE):
            for c in range(CHUNKS):
                for half in range(2):
                    tile_load(step, kind, c, half).start()

    state[1] = jnp.zeros_like(state[1])
    y0_copy.wait()
    src[0, own_slot] = state[0].astype(jnp.bfloat16)
    pl.semaphore_wait(barrier, 7)
    for c in range(CHUNKS):
        send_own(0, c)
    center = c_ref[()]
    half_width = e_ref[()]

    def product(par, slot, off, size, cols):
        rows = pl.ds(pl.multiple_of(slot * piece + off, 128), size)
        return jnp.dot(src[par, slot, :, pl.ds(off, size)], tile[rows, cols], preferred_element_type=jnp.float32)

    def apply_matrix(par, first, combine):
        for step in range(2):
            for index, block in enumerate(BLOCKS[step]):
                if step == 0 and index == 3:

                    @pl.when(far)
                    def _():
                        for kind, c in HELD_BACK:
                            fwd_copy(par, 0, kind, c).start()

                for kind, low, high in block:
                    for c in range(low, high + 1):
                        arrive(par, step, kind, c)
                        if first:
                            for half in range(2):
                                tile_load(step, kind, c, half).wait()

                def total(cols):
                    parts = [product(par, slot_of(step, kind), OFFSETS[low], OFFSETS[high] + WIDTHS[high] - OFFSETS[low], cols) for kind, low, high in block]
                    return sum(parts[1:], parts[0])

                if step == 0 and index == 0:
                    acc[...] = total(slice(None))
                else:
                    acc[...] += total(slice(None))
        for o in range(CHUNKS):
            partial_copy(par, o).start()
        wait_sends(par)
        for o in range(CHUNKS):
            partial_copy(par, o).wait_recv()
            combine(o, acc[:, pl.ds(piece + OFFSETS[o], WIDTHS[o])] + prec[par, :, pl.ds(OFFSETS[o], WIDTHS[o])])
        for o in range(CHUNKS):
            partial_copy(par, o).wait_send()

    def advance(par, first):
        other = 1 - par

        def combine(o, total):
            cols = pl.ds(OFFSETS[o], WIDTHS[o])
            shifted = total - center * state[par, :, cols]
            if first:
                following = shifted / half_width
            else:
                following = 2.0 * shifted / half_width - state[other, :, cols]
            state[other, :, cols] = following
            src[other, own_slot, :, cols] = following.astype(jnp.bfloat16)
            send_own(other, o)

        apply_matrix(par, first, combine)

    advance(0, True)

    def step(t, carry):
        advance(lax.rem(t, 2), False)
        return carry

    lax.fori_loop(1, DEGREE, step, 0)

    y_out[...] = state[0]

    def gram_part(o, total):
        image[:, pl.ds(OFFSETS[o], WIDTHS[o])] = total.astype(jnp.bfloat16)

    apply_matrix(0, False, gram_part)
    gram_part_sum = lax.dot_general(src[0, own_slot], image[...], (((1,), (1,)), ((), ())), preferred_element_type=jnp.float32)
    half = width // 2
    gall[me] = jnp.concatenate([gram_part_sum[:half], gram_part_sum[half:]], axis=1)

    def gram_copy(d):
        other = lax.rem(me + d, 8)
        return remote(gall.at[me], gall.at[me], gsend_sem.at[d], grecv_sem.at[me], (other // 2, lax.rem(other, 2)))

    for d in range(1, 8):
        gram_copy(d).start()
    for d in range(1, 8):
        origin = lax.rem(me + d, 8)
        remote(gall.at[origin], gall.at[origin], gsend_sem.at[d], grecv_sem.at[origin], (chip, core)).wait_recv()
    total = gall[0]
    for d in range(1, 8):
        total = total + gall[d]
    total = total / (8 * piece)
    g_out[:half] = total[:, :width]
    g_out[half:] = total[:, width:]
    for d in range(1, 8):
        gram_copy(d).wait_send()


def solution(mesh):
    def local_filter(mat_tile, y_start, center, half_width):
        piece, width = y_start.shape
        rows, cols = mat_tile.shape
        y_t, gram = pl.pallas_call(
            functools.partial(filter_kernel, piece, width),
            out_shape=(pltpu.VMEM((width, piece), jnp.float32), pltpu.VMEM((width, width), jnp.float32)),
            in_specs=[pl.BlockSpec(memory_space=pl.ANY)] * 2 + [pl.BlockSpec(memory_space=pltpu.SMEM)] * 2,
            out_specs=(pl.BlockSpec(memory_space=pltpu.VMEM),) * 2,
            scratch_shapes=[
                pltpu.VMEM((rows, cols), jnp.bfloat16),
                pltpu.VMEM((2, 5, width, piece), jnp.bfloat16),
                pltpu.VMEM((2, width, piece), jnp.float32),
                pltpu.VMEM((width, cols), jnp.float32),
                pltpu.VMEM((2, width, piece), jnp.float32),
                pltpu.VMEM((8, width // 2, 2 * width), jnp.float32),
                pltpu.VMEM((width, piece), jnp.bfloat16),
                pltpu.SemaphoreType.DMA((2, 2, CHUNKS, 2)),
                pltpu.SemaphoreType.DMA((2, 4, CHUNKS)),
                pltpu.SemaphoreType.DMA((3, CHUNKS)),
                pltpu.SemaphoreType.DMA((2, CHUNKS)),
                pltpu.SemaphoreType.DMA((CHUNKS,)),
                pltpu.SemaphoreType.DMA((2, CHUNKS)),
                pltpu.SemaphoreType.DMA((8,)),
                pltpu.SemaphoreType.DMA((8,)),
                pltpu.SemaphoreType.DMA,
            ],
            compiler_params=pltpu.CompilerParams(collective_id=0, has_side_effects=True, vmem_limit_bytes=56 * 1024 * 1024),
            name="filter",
        )(mat_tile, y_start.T, center, half_width)
        return y_t.T, gram

    return jax.shard_map(local_filter, mesh=mesh, in_specs=(P("row", "col"), P(("col", "row"), None), P(), P()), out_specs=(P(("col", "row"), None), P()), check_vma=False)
```

```python
import functools

import jax
import jax.numpy as jnp
from jax import lax
from jax.experimental import pallas as pl
from jax.experimental.pallas import tpu as pltpu
from jax.sharding import PartitionSpec as P

DEGREE = 8
WIDTHS = (256, 256, 256, 256, 256, 128)
OFFSETS = (0, 256, 512, 768, 1024, 1280)
CHUNKS = len(WIDTHS)
MESH = pl.DeviceIdType.MESH
EARLY, LATE = 0, 1
BLOCKS = (
    (((EARLY, 0, 0),), ((EARLY, 1, 2),), ((LATE, 0, 0), (EARLY, 3, 3)), ((LATE, 1, 1), (EARLY, 4, 5)), ((LATE, 2, 3),), ((LATE, 4, 5),)),
    (((EARLY, 0, 1),), ((EARLY, 2, 3), (LATE, 0, 0)), ((LATE, 1, 1), (EARLY, 4, 5), (LATE, 2, 2)), ((LATE, 3, 5),)),
)


def filter_kernel(piece, width, a_ref, y0_ref, c_ref, e_ref, y_out, g_out, tile, src, state, acc, prec, gall, image, tile_sem, recv_sem, send_sem, fwd_sem, psend_sem, prec_sem, gsend_sem, grecv_sem, y_sem):
    chip = lax.axis_index("col")
    core = lax.axis_index("row")
    me = chip * 2 + core
    sibling = 1 - core
    chip_bit = lax.rem(chip, 2)
    chip_x = chip + 1 - 2 * chip_bit
    chip_y = lax.rem(chip + 2, 4)
    group = chip // 2
    near_int = 1 - lax.abs(core - group)
    near = near_int == 1
    far = near_int == 0

    own_dest = 2 * chip_bit + core
    own_slot = near_int * own_dest + (1 - near_int) * 4
    pair_base = (2 * chip_bit, 2 * (1 - chip_bit))
    fwd_chip = near_int * chip_y + (1 - near_int) * chip_x

    def slot_of(step, kind):
        return pair_base[step] + (core if kind == LATE else sibling)

    def tile_load(step, kind, c, half):
        col = core if half else sibling
        rows = pl.ds(pl.multiple_of(slot_of(step, kind) * piece + OFFSETS[c], 128), WIDTHS[c])
        return pltpu.make_async_copy(
            a_ref.at[rows, pl.ds(pl.multiple_of(col * piece, 128), piece)],
            tile.at[rows, pl.ds(half * piece, piece)],
            tile_sem.at[step, kind, c, half],
        )

    def slot_view(par, slot, c):
        return src.at[par, slot, :, pl.ds(OFFSETS[c], WIDTHS[c])]

    def remote(src_view, dst_view, ssem, rsem, dev):
        return pltpu.make_async_remote_copy(src_ref=src_view, dst_ref=dst_view, send_sem=ssem, recv_sem=rsem, device_id=dev, device_id_type=MESH)

    def own_copy(par, c, d):
        dev = ((chip_x, group), (chip_y, group), (chip, group))[d]
        return remote(slot_view(par, own_slot, c), slot_view(par, own_dest, c), send_sem.at[d, c], recv_sem.at[par, own_dest, c], dev)

    def fwd_copy(par, step, kind, c):
        slot = slot_of(step, kind)
        return remote(slot_view(par, slot, c), slot_view(par, slot, c), fwd_sem.at[kind, c], recv_sem.at[par, slot, c], (fwd_chip, core))

    def wait_slot(par, slot, c):
        view = slot_view(par, slot, c)
        remote(view, view, fwd_sem.at[0, c], recv_sem.at[par, slot, c], (chip, core)).wait_recv()

    def partial_copy(par, o):
        cols = pl.ds(OFFSETS[o], WIDTHS[o])
        return remote(acc.at[:, cols], prec.at[par, :, cols], psend_sem.at[o], prec_sem.at[par, o], (chip, sibling))

    def send_own(par, c):
        own_copy(par, c, 1).start()

        @pl.when(far)
        def _():
            own_copy(par, c, 2).start()

    def send_own_x(par):
        for c in range(CHUNKS):
            own_copy(par, c, 0).start()

    def wait_sends(par):
        for c in range(CHUNKS):
            own_copy(par, c, 0).wait_send()
            own_copy(par, c, 1).wait_send()

            @pl.when(far)
            def _():
                own_copy(par, c, 2).wait_send()

            for kind in (EARLY, LATE):

                @pl.when(near if (c + kind) % 2 == 0 else far)
                def _():
                    fwd_copy(par, 0, kind, c).wait_send()

    def arrive(par, step, kind, c):
        if step == 1:
            wait_slot(par, slot_of(1, kind), c)
            if (c + kind) % 2 == 0:

                @pl.when(near)
                def _():
                    fwd_copy(par, 1, kind, c).start()

            return

        if kind == EARLY:
            wait_slot(par, slot_of(0, kind), c)

        if kind == LATE or (c + kind) % 2 == 1:

            @pl.when(far)
            def _():
                if kind == LATE:
                    wait_slot(par, slot_of(0, kind), c)
                if (c + kind) % 2 == 1:
                    fwd_copy(par, 0, kind, c).start()

    y0_copy = pltpu.make_async_copy(y0_ref, state.at[0], y_sem)
    y0_copy.start()

    barrier = pltpu.get_barrier_semaphore()
    for d in range(1, 8):
        other = lax.rem(me + d, 8)
        pl.semaphore_signal(barrier, inc=1, device_id=(other // 2, lax.rem(other, 2)), device_id_type=MESH)

    for step in range(2):
        for kind in (EARLY, LATE):
            for c in range(CHUNKS):
                for half in range(2):
                    tile_load(step, kind, c, half).start()

    state[1] = jnp.zeros_like(state[1])
    y0_copy.wait()
    src[0, own_slot] = state[0].astype(jnp.bfloat16)
    pl.semaphore_wait(barrier, 7)
    for c in range(CHUNKS):
        send_own(0, c)
    send_own_x(0)
    center = c_ref[()]
    half_width = e_ref[()]

    def product(par, slot, off, size, cols):
        rows = pl.ds(pl.multiple_of(slot * piece + off, 128), size)
        return jnp.dot(src[par, slot, :, pl.ds(off, size)], tile[rows, cols], preferred_element_type=jnp.float32)

    def apply_matrix(par, first, combine, finish):
        for step in range(2):
            for index, block in enumerate(BLOCKS[step]):
                for kind, low, high in block:
                    for c in range(low, high + 1):
                        arrive(par, step, kind, c)
                        if first:
                            for half in range(2):
                                tile_load(step, kind, c, half).wait()

                def total(cols):
                    parts = [product(par, slot_of(step, kind), OFFSETS[low], OFFSETS[high] + WIDTHS[high] - OFFSETS[low], cols) for kind, low, high in block]
                    return sum(parts[1:], parts[0])

                if step == 0 and index == 0:
                    acc[...] = total(slice(None))
                else:
                    acc[...] += total(slice(None))
        for o in range(CHUNKS):
            partial_copy(par, o).start()
        wait_sends(par)
        for o in range(CHUNKS):
            partial_copy(par, o).wait_recv()
            combine(o, acc[:, pl.ds(piece + OFFSETS[o], WIDTHS[o])] + prec[par, :, pl.ds(OFFSETS[o], WIDTHS[o])])
        finish()
        for o in range(CHUNKS):
            partial_copy(par, o).wait_send()

    def advance(par, first):
        other = 1 - par

        def combine(o, total):
            cols = pl.ds(OFFSETS[o], WIDTHS[o])
            shifted = total - center * state[par, :, cols]
            if first:
                following = shifted / half_width
            else:
                following = 2.0 * shifted / half_width - state[other, :, cols]
            state[other, :, cols] = following
            src[other, own_slot, :, cols] = following.astype(jnp.bfloat16)
            send_own(other, o)

        apply_matrix(par, first, combine, lambda: send_own_x(other))

    advance(0, True)

    def step(t, carry):
        advance(lax.rem(t, 2), False)
        return carry

    lax.fori_loop(1, DEGREE, step, 0)

    y_out[...] = state[0]

    def gram_part(o, total):
        image[:, pl.ds(OFFSETS[o], WIDTHS[o])] = total.astype(jnp.bfloat16)

    apply_matrix(0, False, gram_part, lambda: None)
    gram_part_sum = lax.dot_general(src[0, own_slot], image[...], (((1,), (1,)), ((), ())), preferred_element_type=jnp.float32)
    half = width // 2
    gall[me] = jnp.concatenate([gram_part_sum[:half], gram_part_sum[half:]], axis=1)

    def gram_copy(d):
        other = lax.rem(me + d, 8)
        return remote(gall.at[me], gall.at[me], gsend_sem.at[d], grecv_sem.at[me], (other // 2, lax.rem(other, 2)))

    for d in range(1, 8):
        gram_copy(d).start()
    for d in range(1, 8):
        origin = lax.rem(me + d, 8)
        remote(gall.at[origin], gall.at[origin], gsend_sem.at[d], grecv_sem.at[origin], (chip, core)).wait_recv()
    total = gall[0]
    for d in range(1, 8):
        total = total + gall[d]
    total = total / (8 * piece)
    g_out[:half] = total[:, :width]
    g_out[half:] = total[:, width:]
    for d in range(1, 8):
        gram_copy(d).wait_send()


def solution(mesh):
    def local_filter(mat_tile, y_start, center, half_width):
        piece, width = y_start.shape
        rows, cols = mat_tile.shape
        y_t, gram = pl.pallas_call(
            functools.partial(filter_kernel, piece, width),
            out_shape=(pltpu.VMEM((width, piece), jnp.float32), pltpu.VMEM((width, width), jnp.float32)),
            in_specs=[pl.BlockSpec(memory_space=pl.ANY)] * 2 + [pl.BlockSpec(memory_space=pltpu.SMEM)] * 2,
            out_specs=(pl.BlockSpec(memory_space=pltpu.VMEM),) * 2,
            scratch_shapes=[
                pltpu.VMEM((rows, cols), jnp.bfloat16),
                pltpu.VMEM((2, 5, width, piece), jnp.bfloat16),
                pltpu.VMEM((2, width, piece), jnp.float32),
                pltpu.VMEM((width, cols), jnp.float32),
                pltpu.VMEM((2, width, piece), jnp.float32),
                pltpu.VMEM((8, width // 2, 2 * width), jnp.float32),
                pltpu.VMEM((width, piece), jnp.bfloat16),
                pltpu.SemaphoreType.DMA((2, 2, CHUNKS, 2)),
                pltpu.SemaphoreType.DMA((2, 4, CHUNKS)),
                pltpu.SemaphoreType.DMA((3, CHUNKS)),
                pltpu.SemaphoreType.DMA((2, CHUNKS)),
                pltpu.SemaphoreType.DMA((CHUNKS,)),
                pltpu.SemaphoreType.DMA((2, CHUNKS)),
                pltpu.SemaphoreType.DMA((8,)),
                pltpu.SemaphoreType.DMA((8,)),
                pltpu.SemaphoreType.DMA,
            ],
            compiler_params=pltpu.CompilerParams(collective_id=0, has_side_effects=True, vmem_limit_bytes=56 * 1024 * 1024),
            name="filter",
        )(mat_tile, y_start.T, center, half_width)
        return y_t.T, gram

    return jax.shard_map(local_filter, mesh=mesh, in_specs=(P("row", "col"), P(("col", "row"), None), P(), P()), out_specs=(P(("col", "row"), None), P()), check_vma=False)
```

```python
import functools

import jax
import jax.numpy as jnp
from jax import lax
from jax.experimental import pallas as pl
from jax.experimental.pallas import tpu as pltpu
from jax.sharding import PartitionSpec as P

DEGREE = 8
WIDTHS = (256, 256, 256, 256, 256, 128)
OFFSETS = (0, 256, 512, 768, 1024, 1280)
CHUNKS = len(WIDTHS)
MESH = pl.DeviceIdType.MESH
EARLY, LATE = 0, 1
BLOCKS = (
    (((EARLY, 0, 0),), ((EARLY, 1, 2),), ((LATE, 0, 0), (EARLY, 3, 3)), ((LATE, 1, 1), (EARLY, 4, 5)), ((LATE, 2, 3),), ((LATE, 4, 5),)),
    (((EARLY, 0, 1),), ((EARLY, 2, 3), (LATE, 0, 0)), ((LATE, 1, 1), (EARLY, 4, 5), (LATE, 2, 2)), ((LATE, 3, 5),)),
)
NEAR_RELAYS = ((EARLY, 0), (EARLY, 2), (LATE, 1), (LATE, 5))


def filter_kernel(piece, width, a_ref, y0_ref, c_ref, e_ref, y_out, g_out, tile, src, state, acc, prec, gall, image, tile_sem, recv_sem, send_sem, fwd_sem, psend_sem, prec_sem, gsend_sem, grecv_sem, y_sem):
    chip = lax.axis_index("col")
    core = lax.axis_index("row")
    me = chip * 2 + core
    sibling = 1 - core
    chip_bit = lax.rem(chip, 2)
    chip_x = chip + 1 - 2 * chip_bit
    chip_y = lax.rem(chip + 2, 4)
    group = chip // 2
    near_int = 1 - lax.abs(core - group)
    near = near_int == 1
    far = near_int == 0

    own_dest = 2 * chip_bit + core
    own_slot = near_int * own_dest + (1 - near_int) * 4
    pair_base = (2 * chip_bit, 2 * (1 - chip_bit))
    fwd_chip = near_int * chip_y + (1 - near_int) * chip_x

    def slot_of(step, kind):
        return pair_base[step] + (core if kind == LATE else sibling)

    def tile_load(step, kind, c, half):
        col = core if half else sibling
        rows = pl.ds(pl.multiple_of(slot_of(step, kind) * piece + OFFSETS[c], 128), WIDTHS[c])
        return pltpu.make_async_copy(
            a_ref.at[rows, pl.ds(pl.multiple_of(col * piece, 128), piece)],
            tile.at[rows, pl.ds(half * piece, piece)],
            tile_sem.at[step, kind, c, half],
        )

    def slot_view(par, slot, c):
        return src.at[par, slot, :, pl.ds(OFFSETS[c], WIDTHS[c])]

    def remote(src_view, dst_view, ssem, rsem, dev):
        return pltpu.make_async_remote_copy(src_ref=src_view, dst_ref=dst_view, send_sem=ssem, recv_sem=rsem, device_id=dev, device_id_type=MESH)

    def own_copy(par, c, d):
        dev = ((chip_x, group), (chip_y, group), (chip, group))[d]
        return remote(slot_view(par, own_slot, c), slot_view(par, own_dest, c), send_sem.at[d, c], recv_sem.at[par, own_dest, c], dev)

    def fwd_copy(par, step, kind, c):
        slot = slot_of(step, kind)
        return remote(slot_view(par, slot, c), slot_view(par, slot, c), fwd_sem.at[kind, c], recv_sem.at[par, slot, c], (fwd_chip, core))

    def wait_slot(par, slot, c):
        view = slot_view(par, slot, c)
        remote(view, view, fwd_sem.at[0, c], recv_sem.at[par, slot, c], (chip, core)).wait_recv()

    def partial_copy(par, o):
        cols = pl.ds(OFFSETS[o], WIDTHS[o])
        return remote(acc.at[:, cols], prec.at[par, :, cols], psend_sem.at[o], prec_sem.at[par, o], (chip, sibling))

    def send_own(par, c):
        own_copy(par, c, 1).start()

        @pl.when(far)
        def _():
            own_copy(par, c, 2).start()

    def send_own_x(par):
        for c in range(CHUNKS):
            own_copy(par, c, 0).start()

    def wait_sends(par):
        for c in range(CHUNKS):
            own_copy(par, c, 0).wait_send()
            own_copy(par, c, 1).wait_send()

            @pl.when(far)
            def _():
                own_copy(par, c, 2).wait_send()

            for kind in (EARLY, LATE):

                @pl.when(near if (kind, c) in NEAR_RELAYS else far)
                def _():
                    fwd_copy(par, 0, kind, c).wait_send()

    def arrive(par, step, kind, c):
        if step == 1:
            wait_slot(par, slot_of(1, kind), c)
            if (kind, c) in NEAR_RELAYS:

                @pl.when(near)
                def _():
                    fwd_copy(par, 1, kind, c).start()

            return

        if kind == EARLY:
            wait_slot(par, slot_of(0, kind), c)

        if kind == LATE or (kind, c) not in NEAR_RELAYS:

            @pl.when(far)
            def _():
                if kind == LATE:
                    wait_slot(par, slot_of(0, kind), c)
                if (kind, c) not in NEAR_RELAYS:
                    fwd_copy(par, 0, kind, c).start()

    y0_copy = pltpu.make_async_copy(y0_ref, state.at[0], y_sem)
    y0_copy.start()

    barrier = pltpu.get_barrier_semaphore()
    for d in range(1, 8):
        other = lax.rem(me + d, 8)
        pl.semaphore_signal(barrier, inc=1, device_id=(other // 2, lax.rem(other, 2)), device_id_type=MESH)

    for step in range(2):
        for kind in (EARLY, LATE):
            for c in range(CHUNKS):
                for half in range(2):
                    tile_load(step, kind, c, half).start()

    state[1] = jnp.zeros_like(state[1])
    y0_copy.wait()
    src[0, own_slot] = state[0].astype(jnp.bfloat16)
    pl.semaphore_wait(barrier, 7)
    for c in range(CHUNKS):
        send_own(0, c)
    send_own_x(0)
    center = c_ref[()]
    half_width = e_ref[()]

    def product(par, slot, off, size, cols):
        rows = pl.ds(pl.multiple_of(slot * piece + off, 128), size)
        return jnp.dot(src[par, slot, :, pl.ds(off, size)], tile[rows, cols], preferred_element_type=jnp.float32)

    def apply_matrix(par, first, combine, finish):
        for step in range(2):
            for index, block in enumerate(BLOCKS[step]):
                for kind, low, high in block:
                    for c in range(low, high + 1):
                        arrive(par, step, kind, c)
                        if first:
                            for half in range(2):
                                tile_load(step, kind, c, half).wait()

                def total(cols):
                    parts = [product(par, slot_of(step, kind), OFFSETS[low], OFFSETS[high] + WIDTHS[high] - OFFSETS[low], cols) for kind, low, high in block]
                    return sum(parts[1:], parts[0])

                if step == 0 and index == 0:
                    acc[...] = total(slice(None))
                else:
                    acc[...] += total(slice(None))
        for o in range(CHUNKS):
            partial_copy(par, o).start()
        wait_sends(par)
        for o in range(CHUNKS):
            partial_copy(par, o).wait_recv()
            combine(o, acc[:, pl.ds(piece + OFFSETS[o], WIDTHS[o])] + prec[par, :, pl.ds(OFFSETS[o], WIDTHS[o])])
        finish()
        for o in range(CHUNKS):
            partial_copy(par, o).wait_send()

    def advance(par, first):
        other = 1 - par

        def combine(o, total):
            cols = pl.ds(OFFSETS[o], WIDTHS[o])
            shifted = total - center * state[par, :, cols]
            if first:
                following = shifted / half_width
            else:
                following = 2.0 * shifted / half_width - state[other, :, cols]
            state[other, :, cols] = following
            src[other, own_slot, :, cols] = following.astype(jnp.bfloat16)
            send_own(other, o)

        apply_matrix(par, first, combine, lambda: send_own_x(other))

    advance(0, True)

    def step(t, carry):
        advance(lax.rem(t, 2), False)
        return carry

    lax.fori_loop(1, DEGREE, step, 0)

    y_out[...] = state[0]

    def gram_part(o, total):
        image[:, pl.ds(OFFSETS[o], WIDTHS[o])] = total.astype(jnp.bfloat16)

    apply_matrix(0, False, gram_part, lambda: None)
    gram_part_sum = lax.dot_general(src[0, own_slot], image[...], (((1,), (1,)), ((), ())), preferred_element_type=jnp.float32)
    half = width // 2
    gall[me] = jnp.concatenate([gram_part_sum[:half], gram_part_sum[half:]], axis=1)

    def gram_copy(d):
        other = lax.rem(me + d, 8)
        return remote(gall.at[me], gall.at[me], gsend_sem.at[d], grecv_sem.at[me], (other // 2, lax.rem(other, 2)))

    for d in range(1, 8):
        gram_copy(d).start()
    for d in range(1, 8):
        origin = lax.rem(me + d, 8)
        remote(gall.at[origin], gall.at[origin], gsend_sem.at[d], grecv_sem.at[origin], (chip, core)).wait_recv()
    total = gall[0]
    for d in range(1, 8):
        total = total + gall[d]
    total = total / (8 * piece)
    g_out[:half] = total[:, :width]
    g_out[half:] = total[:, width:]
    for d in range(1, 8):
        gram_copy(d).wait_send()


def solution(mesh):
    def local_filter(mat_tile, y_start, center, half_width):
        piece, width = y_start.shape
        rows, cols = mat_tile.shape
        y_t, gram = pl.pallas_call(
            functools.partial(filter_kernel, piece, width),
            out_shape=(pltpu.VMEM((width, piece), jnp.float32), pltpu.VMEM((width, width), jnp.float32)),
            in_specs=[pl.BlockSpec(memory_space=pl.ANY)] * 2 + [pl.BlockSpec(memory_space=pltpu.SMEM)] * 2,
            out_specs=(pl.BlockSpec(memory_space=pltpu.VMEM),) * 2,
            scratch_shapes=[
                pltpu.VMEM((rows, cols), jnp.bfloat16),
                pltpu.VMEM((2, 5, width, piece), jnp.bfloat16),
                pltpu.VMEM((2, width, piece), jnp.float32),
                pltpu.VMEM((width, cols), jnp.float32),
                pltpu.VMEM((2, width, piece), jnp.float32),
                pltpu.VMEM((8, width // 2, 2 * width), jnp.float32),
                pltpu.VMEM((width, piece), jnp.bfloat16),
                pltpu.SemaphoreType.DMA((2, 2, CHUNKS, 2)),
                pltpu.SemaphoreType.DMA((2, 4, CHUNKS)),
                pltpu.SemaphoreType.DMA((3, CHUNKS)),
                pltpu.SemaphoreType.DMA((2, CHUNKS)),
                pltpu.SemaphoreType.DMA((CHUNKS,)),
                pltpu.SemaphoreType.DMA((2, CHUNKS)),
                pltpu.SemaphoreType.DMA((8,)),
                pltpu.SemaphoreType.DMA((8,)),
                pltpu.SemaphoreType.DMA,
            ],
            compiler_params=pltpu.CompilerParams(collective_id=0, has_side_effects=True, vmem_limit_bytes=56 * 1024 * 1024),
            name="filter",
        )(mat_tile, y_start.T, center, half_width)
        return y_t.T, gram

    return jax.shard_map(local_filter, mesh=mesh, in_specs=(P("row", "col"), P(("col", "row"), None), P(), P()), out_specs=(P(("col", "row"), None), P()), check_vma=False)
```

```python
import functools

import jax
import jax.numpy as jnp
from jax import lax
from jax.experimental import pallas as pl
from jax.experimental.pallas import tpu as pltpu
from jax.sharding import PartitionSpec as P

DEGREE = 8
WIDTHS = (256, 256, 256, 256, 256, 128)
OFFSETS = (0, 256, 512, 768, 1024, 1280)
CHUNKS = len(WIDTHS)
MESH = pl.DeviceIdType.MESH
EARLY, LATE = 0, 1
BLOCKS = (
    (((EARLY, 0, 0),), ((EARLY, 1, 2),), ((EARLY, 3, 5),), ((LATE, 0, 1),), ((LATE, 2, 3),), ((LATE, 4, 5),)),
    (((EARLY, 0, 1),), ((EARLY, 2, 3), (LATE, 0, 0)), ((LATE, 1, 1), (EARLY, 4, 5), (LATE, 2, 2)), ((LATE, 3, 5),)),
)
NEAR_RELAYS = ((EARLY, 0), (EARLY, 2), (LATE, 1), (LATE, 5))


def filter_kernel(piece, width, a_ref, y0_ref, c_ref, e_ref, y_out, g_out, tile, src, state, acc, prec, gall, image, tile_sem, recv_sem, send_sem, fwd_sem, psend_sem, prec_sem, gsend_sem, grecv_sem, y_sem):
    chip = lax.axis_index("col")
    core = lax.axis_index("row")
    me = chip * 2 + core
    sibling = 1 - core
    chip_bit = lax.rem(chip, 2)
    chip_x = chip + 1 - 2 * chip_bit
    chip_y = lax.rem(chip + 2, 4)
    group = chip // 2
    near_int = 1 - lax.abs(core - group)
    near = near_int == 1
    far = near_int == 0

    own_dest = 2 * chip_bit + core
    own_slot = near_int * own_dest + (1 - near_int) * 4
    pair_base = (2 * chip_bit, 2 * (1 - chip_bit))
    fwd_chip = near_int * chip_y + (1 - near_int) * chip_x

    def slot_of(step, kind):
        return pair_base[step] + (core if kind == LATE else sibling)

    def tile_load(step, kind, c, half):
        col = core if half else sibling
        rows = pl.ds(pl.multiple_of(slot_of(step, kind) * piece + OFFSETS[c], 128), WIDTHS[c])
        return pltpu.make_async_copy(
            a_ref.at[rows, pl.ds(pl.multiple_of(col * piece, 128), piece)],
            tile.at[rows, pl.ds(half * piece, piece)],
            tile_sem.at[step, kind, c, half],
        )

    def slot_view(par, slot, c):
        return src.at[par, slot, :, pl.ds(OFFSETS[c], WIDTHS[c])]

    def remote(src_view, dst_view, ssem, rsem, dev):
        return pltpu.make_async_remote_copy(src_ref=src_view, dst_ref=dst_view, send_sem=ssem, recv_sem=rsem, device_id=dev, device_id_type=MESH)

    def own_copy(par, c, d):
        dev = ((chip_x, group), (chip_y, group), (chip, group))[d]
        return remote(slot_view(par, own_slot, c), slot_view(par, own_dest, c), send_sem.at[d, c], recv_sem.at[par, own_dest, c], dev)

    def fwd_copy(par, step, kind, c):
        slot = slot_of(step, kind)
        return remote(slot_view(par, slot, c), slot_view(par, slot, c), fwd_sem.at[kind, c], recv_sem.at[par, slot, c], (fwd_chip, core))

    def wait_slot(par, slot, c):
        view = slot_view(par, slot, c)
        remote(view, view, fwd_sem.at[0, c], recv_sem.at[par, slot, c], (chip, core)).wait_recv()

    def partial_copy(par, o):
        cols = pl.ds(OFFSETS[o], WIDTHS[o])
        return remote(acc.at[:, cols], prec.at[par, :, cols], psend_sem.at[o], prec_sem.at[par, o], (chip, sibling))

    def send_own(par, c):
        own_copy(par, c, 1).start()

        @pl.when(far)
        def _():
            own_copy(par, c, 2).start()

    def send_own_x(par):
        for c in range(CHUNKS):
            own_copy(par, c, 0).start()

    def wait_sends(par):
        for c in range(CHUNKS):
            own_copy(par, c, 0).wait_send()
            own_copy(par, c, 1).wait_send()

            @pl.when(far)
            def _():
                own_copy(par, c, 2).wait_send()

            for kind in (EARLY, LATE):

                @pl.when(near if (kind, c) in NEAR_RELAYS else far)
                def _():
                    fwd_copy(par, 0, kind, c).wait_send()

    def arrive(par, step, kind, c):
        if step == 1:
            wait_slot(par, slot_of(1, kind), c)
            if (kind, c) in NEAR_RELAYS:

                @pl.when(near)
                def _():
                    fwd_copy(par, 1, kind, c).start()

            return

        if kind == EARLY:
            wait_slot(par, slot_of(0, kind), c)

        if kind == LATE or (kind, c) not in NEAR_RELAYS:

            @pl.when(far)
            def _():
                if kind == LATE:
                    wait_slot(par, slot_of(0, kind), c)
                if (kind, c) not in NEAR_RELAYS:
                    fwd_copy(par, 0, kind, c).start()

    y0_copy = pltpu.make_async_copy(y0_ref, state.at[0], y_sem)
    y0_copy.start()

    barrier = pltpu.get_barrier_semaphore()
    for d in range(1, 8):
        other = lax.rem(me + d, 8)
        pl.semaphore_signal(barrier, inc=1, device_id=(other // 2, lax.rem(other, 2)), device_id_type=MESH)

    for step in range(2):
        for kind in (EARLY, LATE):
            for c in range(CHUNKS):
                for half in range(2):
                    tile_load(step, kind, c, half).start()

    state[1] = jnp.zeros_like(state[1])
    y0_copy.wait()
    src[0, own_slot] = state[0].astype(jnp.bfloat16)
    pl.semaphore_wait(barrier, 7)
    for c in range(CHUNKS):
        send_own(0, c)
    send_own_x(0)
    center = c_ref[()]
    half_width = e_ref[()]

    def product(par, slot, off, size, cols):
        rows = pl.ds(pl.multiple_of(slot * piece + off, 128), size)
        return jnp.dot(src[par, slot, :, pl.ds(off, size)], tile[rows, cols], preferred_element_type=jnp.float32)

    def apply_matrix(par, first, combine, finish):
        for step in range(2):
            for index, block in enumerate(BLOCKS[step]):
                for kind, low, high in block:
                    for c in range(low, high + 1):
                        arrive(par, step, kind, c)
                        if first:
                            for half in range(2):
                                tile_load(step, kind, c, half).wait()

                def total(cols):
                    parts = [product(par, slot_of(step, kind), OFFSETS[low], OFFSETS[high] + WIDTHS[high] - OFFSETS[low], cols) for kind, low, high in block]
                    return sum(parts[1:], parts[0])

                if step == 0 and index == 0:
                    acc[...] = total(slice(None))
                else:
                    acc[...] += total(slice(None))
        for o in range(CHUNKS):
            partial_copy(par, o).start()
        wait_sends(par)
        for o in range(CHUNKS):
            partial_copy(par, o).wait_recv()
            combine(o, acc[:, pl.ds(piece + OFFSETS[o], WIDTHS[o])] + prec[par, :, pl.ds(OFFSETS[o], WIDTHS[o])])
        finish()
        for o in range(CHUNKS):
            partial_copy(par, o).wait_send()

    def advance(par, first):
        other = 1 - par

        def combine(o, total):
            cols = pl.ds(OFFSETS[o], WIDTHS[o])
            shifted = total - center * state[par, :, cols]
            if first:
                following = shifted / half_width
            else:
                following = 2.0 * shifted / half_width - state[other, :, cols]
            state[other, :, cols] = following
            src[other, own_slot, :, cols] = following.astype(jnp.bfloat16)
            send_own(other, o)

        apply_matrix(par, first, combine, lambda: send_own_x(other))

    advance(0, True)

    def step(t, carry):
        advance(lax.rem(t, 2), False)
        return carry

    lax.fori_loop(1, DEGREE, step, 0)

    y_out[...] = state[0]

    def gram_part(o, total):
        image[:, pl.ds(OFFSETS[o], WIDTHS[o])] = total.astype(jnp.bfloat16)

    apply_matrix(0, False, gram_part, lambda: None)
    gram_part_sum = lax.dot_general(src[0, own_slot], image[...], (((1,), (1,)), ((), ())), preferred_element_type=jnp.float32)
    half = width // 2
    gall[me] = jnp.concatenate([gram_part_sum[:half], gram_part_sum[half:]], axis=1)

    def gram_copy(d):
        other = lax.rem(me + d, 8)
        return remote(gall.at[me], gall.at[me], gsend_sem.at[d], grecv_sem.at[me], (other // 2, lax.rem(other, 2)))

    for d in range(1, 8):
        gram_copy(d).start()
    for d in range(1, 8):
        origin = lax.rem(me + d, 8)
        remote(gall.at[origin], gall.at[origin], gsend_sem.at[d], grecv_sem.at[origin], (chip, core)).wait_recv()
    total = gall[0]
    for d in range(1, 8):
        total = total + gall[d]
    total = total / (8 * piece)
    g_out[:half] = total[:, :width]
    g_out[half:] = total[:, width:]
    for d in range(1, 8):
        gram_copy(d).wait_send()


def solution(mesh):
    def local_filter(mat_tile, y_start, center, half_width):
        piece, width = y_start.shape
        rows, cols = mat_tile.shape
        y_t, gram = pl.pallas_call(
            functools.partial(filter_kernel, piece, width),
            out_shape=(pltpu.VMEM((width, piece), jnp.float32), pltpu.VMEM((width, width), jnp.float32)),
            in_specs=[pl.BlockSpec(memory_space=pl.ANY)] * 2 + [pl.BlockSpec(memory_space=pltpu.SMEM)] * 2,
            out_specs=(pl.BlockSpec(memory_space=pltpu.VMEM),) * 2,
            scratch_shapes=[
                pltpu.VMEM((rows, cols), jnp.bfloat16),
                pltpu.VMEM((2, 5, width, piece), jnp.bfloat16),
                pltpu.VMEM((2, width, piece), jnp.float32),
                pltpu.VMEM((width, cols), jnp.float32),
                pltpu.VMEM((2, width, piece), jnp.float32),
                pltpu.VMEM((8, width // 2, 2 * width), jnp.float32),
                pltpu.VMEM((width, piece), jnp.bfloat16),
                pltpu.SemaphoreType.DMA((2, 2, CHUNKS, 2)),
                pltpu.SemaphoreType.DMA((2, 4, CHUNKS)),
                pltpu.SemaphoreType.DMA((3, CHUNKS)),
                pltpu.SemaphoreType.DMA((2, CHUNKS)),
                pltpu.SemaphoreType.DMA((CHUNKS,)),
                pltpu.SemaphoreType.DMA((2, CHUNKS)),
                pltpu.SemaphoreType.DMA((8,)),
                pltpu.SemaphoreType.DMA((8,)),
                pltpu.SemaphoreType.DMA,
            ],
            compiler_params=pltpu.CompilerParams(collective_id=0, has_side_effects=True, vmem_limit_bytes=56 * 1024 * 1024),
            name="filter",
        )(mat_tile, y_start.T, center, half_width)
        return y_t.T, gram

    return jax.shard_map(local_filter, mesh=mesh, in_specs=(P("row", "col"), P(("col", "row"), None), P(), P()), out_specs=(P(("col", "row"), None), P()), check_vma=False)
```

```python
import functools

import jax
import jax.numpy as jnp
from jax import lax
from jax.experimental import pallas as pl
from jax.experimental.pallas import tpu as pltpu
from jax.sharding import PartitionSpec as P

DEGREE = 8
WIDTHS = (256, 256, 256, 256, 256, 128)
OFFSETS = (0, 256, 512, 768, 1024, 1280)
CHUNKS = len(WIDTHS)
MESH = pl.DeviceIdType.MESH
EARLY, LATE = 0, 1
BLOCKS = (
    (((EARLY, 0, 0),), ((EARLY, 1, 2),), ((LATE, 0, 0), (EARLY, 3, 3)), ((LATE, 1, 1), (EARLY, 4, 5)), ((LATE, 2, 3),), ((LATE, 4, 5),)),
    (((EARLY, 0, 1),), ((EARLY, 2, 3), (LATE, 0, 0)), ((LATE, 1, 1), (EARLY, 4, 5), (LATE, 2, 2)), ((LATE, 3, 5),)),
)
NEAR_RELAYS = ((EARLY, 0), (EARLY, 2), (LATE, 1), (LATE, 5))


def filter_kernel(piece, width, a_ref, y0_ref, c_ref, e_ref, y_out, g_out, tile, src, state, acc, prec, gall, image, tile_sem, recv_sem, send_sem, fwd_sem, psend_sem, prec_sem, gsend_sem, grecv_sem, y_sem):
    chip = lax.axis_index("col")
    core = lax.axis_index("row")
    me = chip * 2 + core
    sibling = 1 - core
    chip_bit = lax.rem(chip, 2)
    chip_x = chip + 1 - 2 * chip_bit
    chip_y = lax.rem(chip + 2, 4)
    group = chip // 2
    near_int = 1 - lax.abs(core - group)
    near = near_int == 1
    far = near_int == 0

    own_dest = 2 * chip_bit + core
    own_slot = near_int * own_dest + (1 - near_int) * 4
    pair_base = (2 * chip_bit, 2 * (1 - chip_bit))
    fwd_chip = near_int * chip_y + (1 - near_int) * chip_x

    def slot_of(step, kind):
        return pair_base[step] + (core if kind == LATE else sibling)

    def tile_load(step, kind, c, half):
        col = core if half else sibling
        rows = pl.ds(pl.multiple_of(slot_of(step, kind) * piece + OFFSETS[c], 128), WIDTHS[c])
        return pltpu.make_async_copy(
            a_ref.at[rows, pl.ds(pl.multiple_of(col * piece, 128), piece)],
            tile.at[rows, pl.ds(half * piece, piece)],
            tile_sem.at[step, kind, c],
        )

    def wait_tile(step, kind, c):
        rows = pl.ds(pl.multiple_of(slot_of(step, kind) * piece + OFFSETS[c], 128), WIDTHS[c])
        pltpu.make_async_copy(a_ref.at[rows], tile.at[rows], tile_sem.at[step, kind, c]).wait()

    def slot_view(par, slot, c):
        return src.at[par, slot, :, pl.ds(OFFSETS[c], WIDTHS[c])]

    def remote(src_view, dst_view, ssem, rsem, dev):
        return pltpu.make_async_remote_copy(src_ref=src_view, dst_ref=dst_view, send_sem=ssem, recv_sem=rsem, device_id=dev, device_id_type=MESH)

    def own_copy(par, c, d):
        dev = ((chip_x, group), (chip_y, group), (chip, group))[d]
        return remote(slot_view(par, own_slot, c), slot_view(par, own_dest, c), send_sem.at[d, c], recv_sem.at[par, own_dest, c], dev)

    def fwd_copy(par, step, kind, c):
        slot = slot_of(step, kind)
        return remote(slot_view(par, slot, c), slot_view(par, slot, c), fwd_sem.at[kind, c], recv_sem.at[par, slot, c], (fwd_chip, core))

    def wait_slot(par, slot, c):
        view = slot_view(par, slot, c)
        remote(view, view, fwd_sem.at[0, c], recv_sem.at[par, slot, c], (chip, core)).wait_recv()

    def partial_copy(par, o):
        cols = pl.ds(OFFSETS[o], WIDTHS[o])
        return remote(acc.at[:, cols], prec.at[par, :, cols], psend_sem.at[o], prec_sem.at[par, o], (chip, sibling))

    def send_own(par, c):
        own_copy(par, c, 1).start()

        @pl.when(far)
        def _():
            own_copy(par, c, 2).start()

    def send_own_x(par):
        for c in range(CHUNKS):
            own_copy(par, c, 0).start()

    def wait_sends(par):
        for c in range(CHUNKS):
            own_copy(par, c, 0).wait_send()
            own_copy(par, c, 1).wait_send()

            @pl.when(far)
            def _():
                own_copy(par, c, 2).wait_send()

            for kind in (EARLY, LATE):

                @pl.when(near if (kind, c) in NEAR_RELAYS else far)
                def _():
                    fwd_copy(par, 0, kind, c).wait_send()

    def arrive(par, step, kind, c):
        if step == 1:
            wait_slot(par, slot_of(1, kind), c)
            if (kind, c) in NEAR_RELAYS:

                @pl.when(near)
                def _():
                    fwd_copy(par, 1, kind, c).start()

            return

        if kind == EARLY:
            wait_slot(par, slot_of(0, kind), c)

        if kind == LATE or (kind, c) not in NEAR_RELAYS:

            @pl.when(far)
            def _():
                if kind == LATE:
                    wait_slot(par, slot_of(0, kind), c)
                if (kind, c) not in NEAR_RELAYS:
                    fwd_copy(par, 0, kind, c).start()

    y0_copy = pltpu.make_async_copy(y0_ref, state.at[0], y_sem)
    y0_copy.start()

    barrier = pltpu.get_barrier_semaphore()
    for d in range(1, 8):
        other = lax.rem(me + d, 8)
        pl.semaphore_signal(barrier, inc=1, device_id=(other // 2, lax.rem(other, 2)), device_id_type=MESH)

    for step in range(2):
        for kind in (EARLY, LATE):
            for c in range(CHUNKS):
                for half in range(2):
                    tile_load(step, kind, c, half).start()

    state[1] = jnp.zeros_like(state[1])
    y0_copy.wait()
    src[0, own_slot] = state[0].astype(jnp.bfloat16)
    pl.semaphore_wait(barrier, 7)
    for c in range(CHUNKS):
        send_own(0, c)
    send_own_x(0)
    center = c_ref[()]
    half_width = e_ref[()]

    def product(par, slot, off, size, cols):
        rows = pl.ds(pl.multiple_of(slot * piece + off, 128), size)
        return jnp.dot(src[par, slot, :, pl.ds(off, size)], tile[rows, cols], preferred_element_type=jnp.float32)

    def apply_matrix(par, first, combine, finish):
        for step in range(2):
            for index, block in enumerate(BLOCKS[step]):
                for kind, low, high in block:
                    for c in range(low, high + 1):
                        arrive(par, step, kind, c)
                        if first:
                            wait_tile(step, kind, c)

                def total(cols):
                    parts = [product(par, slot_of(step, kind), OFFSETS[low], OFFSETS[high] + WIDTHS[high] - OFFSETS[low], cols) for kind, low, high in block]
                    return sum(parts[1:], parts[0])

                if step == 0 and index == 0:
                    acc[...] = total(slice(None))
                else:
                    acc[...] += total(slice(None))
        for o in range(CHUNKS):
            partial_copy(par, o).start()
        wait_sends(par)
        for o in range(CHUNKS):
            partial_copy(par, o).wait_recv()
            combine(o, acc[:, pl.ds(piece + OFFSETS[o], WIDTHS[o])] + prec[par, :, pl.ds(OFFSETS[o], WIDTHS[o])])
        finish()
        for o in range(CHUNKS):
            partial_copy(par, o).wait_send()

    def advance(par, first):
        other = 1 - par

        def combine(o, total):
            cols = pl.ds(OFFSETS[o], WIDTHS[o])
            shifted = total - center * state[par, :, cols]
            if first:
                following = shifted / half_width
            else:
                following = 2.0 * shifted / half_width - state[other, :, cols]
            state[other, :, cols] = following
            src[other, own_slot, :, cols] = following.astype(jnp.bfloat16)
            send_own(other, o)

        apply_matrix(par, first, combine, lambda: send_own_x(other))

    advance(0, True)

    def step(t, carry):
        advance(lax.rem(t, 2), False)
        return carry

    lax.fori_loop(1, DEGREE, step, 0)

    y_out[...] = state[0]

    def gram_part(o, total):
        image[:, pl.ds(OFFSETS[o], WIDTHS[o])] = total.astype(jnp.bfloat16)

    apply_matrix(0, False, gram_part, lambda: None)
    gram_part_sum = lax.dot_general(src[0, own_slot], image[...], (((1,), (1,)), ((), ())), preferred_element_type=jnp.float32)
    half = width // 2
    gall[me] = jnp.concatenate([gram_part_sum[:half], gram_part_sum[half:]], axis=1)

    def gram_copy(d):
        other = lax.rem(me + d, 8)
        return remote(gall.at[me], gall.at[me], gsend_sem.at[d], grecv_sem.at[me], (other // 2, lax.rem(other, 2)))

    for d in range(1, 8):
        gram_copy(d).start()
    for d in range(1, 8):
        origin = lax.rem(me + d, 8)
        remote(gall.at[origin], gall.at[origin], gsend_sem.at[d], grecv_sem.at[origin], (chip, core)).wait_recv()
    total = gall[0]
    for d in range(1, 8):
        total = total + gall[d]
    total = total / (8 * piece)
    g_out[:half] = total[:, :width]
    g_out[half:] = total[:, width:]
    for d in range(1, 8):
        gram_copy(d).wait_send()


def solution(mesh):
    def local_filter(mat_tile, y_start, center, half_width):
        piece, width = y_start.shape
        rows, cols = mat_tile.shape
        y_t, gram = pl.pallas_call(
            functools.partial(filter_kernel, piece, width),
            out_shape=(pltpu.VMEM((width, piece), jnp.float32), pltpu.VMEM((width, width), jnp.float32)),
            in_specs=[pl.BlockSpec(memory_space=pl.ANY)] * 2 + [pl.BlockSpec(memory_space=pltpu.SMEM)] * 2,
            out_specs=(pl.BlockSpec(memory_space=pltpu.VMEM),) * 2,
            scratch_shapes=[
                pltpu.VMEM((rows, cols), jnp.bfloat16),
                pltpu.VMEM((2, 5, width, piece), jnp.bfloat16),
                pltpu.VMEM((2, width, piece), jnp.float32),
                pltpu.VMEM((width, cols), jnp.float32),
                pltpu.VMEM((2, width, piece), jnp.float32),
                pltpu.VMEM((8, width // 2, 2 * width), jnp.float32),
                pltpu.VMEM((width, piece), jnp.bfloat16),
                pltpu.SemaphoreType.DMA((2, 2, CHUNKS)),
                pltpu.SemaphoreType.DMA((2, 4, CHUNKS)),
                pltpu.SemaphoreType.DMA((3, CHUNKS)),
                pltpu.SemaphoreType.DMA((2, CHUNKS)),
                pltpu.SemaphoreType.DMA((CHUNKS,)),
                pltpu.SemaphoreType.DMA((2, CHUNKS)),
                pltpu.SemaphoreType.DMA((8,)),
                pltpu.SemaphoreType.DMA((8,)),
                pltpu.SemaphoreType.DMA,
            ],
            compiler_params=pltpu.CompilerParams(collective_id=0, has_side_effects=True, vmem_limit_bytes=56 * 1024 * 1024),
            name="filter",
        )(mat_tile, y_start.T, center, half_width)
        return y_t.T, gram

    return jax.shard_map(local_filter, mesh=mesh, in_specs=(P("row", "col"), P(("col", "row"), None), P(), P()), out_specs=(P(("col", "row"), None), P()), check_vma=False)
```
